8 devices in a mesh: dp: 1 (over z), sp: 8 (over y, x, core).
Axes of the slice: x: 2, y: 2, z: 1, core: 2. Of those that a mesh axis runs over, the one named last changes fastest.
Arguments:
- hidden: bfloat16 [16, 128, 2560], P('dp', 'sp')
- attn_norm: bfloat16 [2560], replicated
- w_q: bfloat16 [2560, 32, 128], replicated
- w_k: bfloat16 [2560, 8, 128], replicated
- w_v: bfloat16 [2560, 8, 128], replicated
- w_o: bfloat16 [32, 128, 2560], replicated
- mlp_norm: bfloat16 [2560], replicated
- w_gate: bfloat16 [2560, 9728], replicated
- w_up: bfloat16 [2560, 9728], replicated
- w_down: bfloat16 [9728, 2560], replicated
- mamba_norm: bfloat16 [2560], replicated
- w_in_x: bfloat16 [2560, 5120], replicated
- w_in_z: bfloat16 [2560, 5120], replicated
- conv_w: bfloat16 [4, 5120], replicated
- conv_b: bfloat16 [5120], replicated
- w_xproj: bfloat16 [5120, 192], replicated
- dt_norm: float32 [160], replicated
- b_norm: float32 [16], replicated
- c_norm: float32 [16], replicated
- w_dt: bfloat16 [160, 5120], replicated
- dt_bias: float32 [5120], replicated
- a_log: float32 [5120, 16], replicated
- d_skip: float32 [5120], replicated
- w_out: bfloat16 [5120, 2560], replicated
Outputs:
- output: bfloat16 [16, 128, 2560], P('dp', 'sp')
All inputs are finite; a program needn't handle non-finite values.
Results may differ from the reference program's by a relative error of at most 0.02.
Values are sent between devices in bfloat16 or wider.
A program may use at most 1.25 GiB of HBM per device.

```python
import jax
import jax.numpy as jnp
from jax import lax

BATCH = 16
TOK_DEV = 16
SEQ = 128
D = 2560
HEADS = 32
KV_HEADS = 8
HEAD = 128
FF = 9728
INNER = 5120
STATE = 16
DT_RANK = 160
CONV = 4
EPS = 1e-6


def setup_inputs(seed: int = 0, part: int = 0) -> dict:
    key_list = jax.random.split(jax.random.key(seed), 24)
    part_key = jax.random.fold_in(key_list[0], part)

    def normal(key_idx, arr_shape, std_dev):
        return jax.random.normal(key_list[key_idx], arr_shape, jnp.float32) * std_dev

    def uniform(key_idx, arr_shape, lower_b, upper_b):
        return jax.random.uniform(key_list[key_idx], arr_shape, jnp.float32, lower_b, upper_b)

    qk_scale = 1.5 * D ** -0.5
    return {
        "hidden": jax.random.normal(part_key, (BATCH, SEQ, D), jnp.float32).astype(jnp.bfloat16),
        "attn_norm": uniform(1, (D,), 0.5, 1.5).astype(jnp.bfloat16),
        "w_q": normal(2, (D, HEADS, HEAD), qk_scale).astype(jnp.bfloat16),
        "w_k": normal(3, (D, KV_HEADS, HEAD), qk_scale).astype(jnp.bfloat16),
        "w_v": normal(4, (D, KV_HEADS, HEAD), D ** -0.5).astype(jnp.bfloat16),
        "w_o": normal(5, (HEADS, HEAD, D), (HEADS * HEAD) ** -0.5).astype(jnp.bfloat16),
        "mlp_norm": uniform(6, (D,), 0.5, 1.5).astype(jnp.bfloat16),
        "w_gate": normal(7, (D, FF), D ** -0.5).astype(jnp.bfloat16),
        "w_up": normal(8, (D, FF), D ** -0.5).astype(jnp.bfloat16),
        "w_down": normal(9, (FF, D), FF ** -0.5).astype(jnp.bfloat16),
        "mamba_norm": uniform(10, (D,), 0.5, 1.5).astype(jnp.bfloat16),
        "w_in_x": normal(11, (D, INNER), D ** -0.5).astype(jnp.bfloat16),
        "w_in_z": normal(12, (D, INNER), D ** -0.5).astype(jnp.bfloat16),
        "conv_w": normal(13, (CONV, INNER), 0.5).astype(jnp.bfloat16),
        "conv_b": normal(14, (INNER,), 0.3).astype(jnp.bfloat16),
        "w_xproj": normal(15, (INNER, DT_RANK + 2 * STATE), INNER ** -0.5).astype(jnp.bfloat16),
        "dt_norm": uniform(16, (DT_RANK,), 0.5, 1.5),
        "b_norm": uniform(17, (STATE,), 0.5, 1.5) * TOK_DEV ** 0.5,
        "c_norm": uniform(18, (STATE,), 0.5, 1.5),
        "w_dt": normal(19, (DT_RANK, INNER), DT_RANK ** -0.5).astype(jnp.bfloat16),
        "dt_bias": jnp.log(uniform(20, (INNER,), 0.25, 1.0) / TOK_DEV),
        "a_log": jnp.log(uniform(21, (INNER, STATE), 0.3, 1.5)),
        "d_skip": uniform(22, (INNER,), -1.5, 1.5),
        "w_out": normal(23, (INNER, D), INNER ** -0.5).astype(jnp.bfloat16),
    }


def rms_scale(values, gain_vec):
    values_f = values.astype(jnp.float32)
    inv_rms = lax.rsqrt(jnp.mean(values_f * values_f, axis=-1, keepdims=True) + EPS)
    return values_f * inv_rms * gain_vec.astype(jnp.float32)


def attention_layer(hidden, attn_norm, w_q, w_k, w_v, w_o):
    n_batch, seq_len, model_dim = hidden.shape
    groups = HEADS // KV_HEADS
    normed = rms_scale(hidden, attn_norm).astype(jnp.bfloat16).reshape(n_batch * seq_len, model_dim)
    queries = jnp.dot(normed, w_q.reshape(model_dim, HEADS * HEAD), preferred_element_type=jnp.float32).astype(jnp.bfloat16)
    key_proj = jnp.dot(normed, w_k.reshape(model_dim, KV_HEADS * HEAD), preferred_element_type=jnp.float32).astype(jnp.bfloat16)
    val_proj = jnp.dot(normed, w_v.reshape(model_dim, KV_HEADS * HEAD), preferred_element_type=jnp.float32).astype(jnp.bfloat16)
    queries = queries.reshape(n_batch, seq_len, KV_HEADS, groups, HEAD).transpose(2, 0, 1, 3, 4)
    key_proj = key_proj.reshape(n_batch, seq_len, KV_HEADS, HEAD).transpose(2, 0, 1, 3)
    val_proj = val_proj.reshape(n_batch, seq_len, KV_HEADS, HEAD).transpose(2, 0, 1, 3)
    causal = jnp.arange(seq_len)[:, None] >= jnp.arange(seq_len)[None, :]

    def one_group(operands):
        q_grp, k_grp, v_grp = operands
        scores = jnp.einsum("bqgd,bsd->bgqs", q_grp.astype(jnp.float32), k_grp.astype(jnp.float32)) * HEAD ** -0.5
        scores = jnp.where(causal, scores, -jnp.inf)
        attn_prob = jax.nn.softmax(scores, axis=-1).astype(jnp.bfloat16)
        return jnp.einsum("bgqs,bsd->bqgd", attn_prob.astype(jnp.float32), v_grp.astype(jnp.float32)).astype(jnp.bfloat16)

    attn_out = lax.map(one_group, (queries, key_proj, val_proj))
    attn_out = attn_out.transpose(1, 2, 0, 3, 4).reshape(n_batch * seq_len, HEADS * HEAD)
    proj_out = jnp.dot(attn_out, w_o.reshape(HEADS * HEAD, model_dim), preferred_element_type=jnp.float32)
    return (hidden.astype(jnp.float32) + proj_out.reshape(n_batch, seq_len, model_dim)).astype(jnp.bfloat16)


def mlp_layer(hidden, mlp_norm, w_gate, w_up, w_down):
    model_dim = hidden.shape[-1]
    normed = rms_scale(hidden, mlp_norm).astype(jnp.bfloat16).reshape(-1, model_dim)
    gate_pre = jnp.dot(normed, w_gate, preferred_element_type=jnp.float32)
    up_proj = jnp.dot(normed, w_up, preferred_element_type=jnp.float32)
    act_val = (jax.nn.silu(gate_pre) * up_proj).astype(jnp.bfloat16)
    down_out = jnp.dot(act_val, w_down, preferred_element_type=jnp.float32)
    return (hidden.astype(jnp.float32) + down_out.reshape(hidden.shape)).astype(jnp.bfloat16)


def mamba_mixer(hidden, mamba_norm, w_in_x, w_in_z, conv_w, conv_b, w_xproj, dt_norm, b_norm, c_norm, w_dt, dt_bias, a_log, d_skip, w_out):
    n_batch, seq_len, model_dim = hidden.shape
    normed = rms_scale(hidden, mamba_norm).astype(jnp.bfloat16).astype(jnp.float32)
    x_inner = jnp.einsum("btd,de->tbe", normed, w_in_x.astype(jnp.float32)).astype(jnp.bfloat16)
    z_gate = jnp.einsum("btd,de->tbe", normed, w_in_z.astype(jnp.float32)).astype(jnp.bfloat16)
    padded = jnp.concatenate([jnp.zeros((CONV - 1, n_batch, INNER), jnp.bfloat16), x_inner], axis=0)
    conv_acc = conv_b.astype(jnp.float32)
    for tap_idx in range(CONV):
        conv_acc = conv_acc + padded[tap_idx:tap_idx + seq_len].astype(jnp.float32) * conv_w[tap_idx].astype(jnp.float32)
    x_conv = jax.nn.silu(conv_acc).astype(jnp.bfloat16)
    x_dbl = jnp.einsum("tbe,er->tbr", x_conv.astype(jnp.float32), w_xproj.astype(jnp.float32))
    dt_in = rms_scale(x_dbl[..., :DT_RANK], dt_norm).astype(jnp.bfloat16)
    b_mat = rms_scale(x_dbl[..., DT_RANK:DT_RANK + STATE], b_norm)
    c_mat = rms_scale(x_dbl[..., DT_RANK + STATE:], c_norm)
    step_size = jax.nn.softplus(jnp.einsum("tbr,re->tbe", dt_in.astype(jnp.float32), w_dt.astype(jnp.float32)) + dt_bias)
    a_mat = -jnp.exp(a_log)

    def scan_step(ssm_state, inputs):
        step_t, x_t, b_t, c_t = inputs
        decay_t = jnp.exp(step_t[:, :, None] * a_mat)
        ssm_state = decay_t * ssm_state + (step_t * x_t.astype(jnp.float32))[:, :, None] * b_t[:, None, :]
        return ssm_state, jnp.sum(ssm_state * c_t[:, None, :], axis=-1)

    zero_state = jnp.zeros((n_batch, INNER, STATE), jnp.float32)
    y_seq = lax.scan(scan_step, zero_state, (step_size, x_conv, b_mat, c_mat))[1]
    gated_y = ((y_seq + d_skip * x_conv.astype(jnp.float32)) * jax.nn.silu(z_gate.astype(jnp.float32))).astype(jnp.bfloat16)
    mamba_out = jnp.einsum("tbe,ed->btd", gated_y.astype(jnp.float32), w_out.astype(jnp.float32))
    return (hidden.astype(jnp.float32) + mamba_out).astype(jnp.bfloat16)


def reference(hidden, attn_norm, w_q, w_k, w_v, w_o, mlp_norm, w_gate, w_up, w_down, mamba_norm, w_in_x, w_in_z, conv_w, conv_b, w_xproj, dt_norm, b_norm, c_norm, w_dt, dt_bias, a_log, d_skip, w_out):
    after_attn = attention_layer(hidden, attn_norm, w_q, w_k, w_v, w_o)
    after_mlp = mlp_layer(after_attn, mlp_norm, w_gate, w_up, w_down)
    return mamba_mixer(after_mlp, mamba_norm, w_in_x, w_in_z, conv_w, conv_b, w_xproj, dt_norm, b_norm, c_norm, w_dt, dt_bias, a_log, d_skip, w_out)
```

```python
import functools
import math
import jax
import jax.numpy as jnp
from jax import lax
from jax.experimental import pallas as pl
from jax.experimental.pallas import tpu as pltpu
from jax.sharding import PartitionSpec as P

EPS = 1e-6
CONV = 4
SLOTS = 9
WN = 512
PITCH = 41
F32 = jnp.float32
BF16 = jnp.bfloat16
LOG2E = math.log2(math.e)


def rms_scale(values, gain_vec):
    values_f = values.astype(F32)
    inv_rms = lax.rsqrt(jnp.mean(values_f * values_f, axis=-1, keepdims=True) + EPS)
    return values_f * inv_rms * gain_vec.astype(F32)


def silu(v):
    half = 0.5 * v
    return half + half * jnp.tanh(half)


def block_kernel(q_hbm, k_hbm, v_hbm, x_hbm, wo, wg, wu, wd, wx, wz, wxp_hbm, wdt_hbm, wout,
                 norms, chan, gains, dskip, a2, out_ref,
                 ring, qo, kbuf, vbuf, h, a, act, xc, zg, delta, xs, bb, cb, wxp, wdt,
                 ring_sem, in_sem):
    rows, dim = h.shape
    seq = 128
    n_seq = rows // seq
    inner = wx.shape[1]
    ff = wg.shape[1]
    qdim = wo.shape[0]
    kv_heads = kbuf.shape[1] // 128
    groups = qdim // kbuf.shape[1]
    lanes = inner // 128
    n_state = a2.shape[0] // lanes
    dt_rank = wdt.shape[0]
    unit = ring.shape[1]

    def chunks(total):
        return [(s, min(unit, total - s)) for s in range(0, total, unit)]

    def cols(t):
        return pl.ds(pl.multiple_of(t * WN, WN), WN)

    segs = []
    base = 0

    def add_seg(n_tiles, parts):
        nonlocal base
        first = base
        base = first + n_tiles * len(parts)
        segs.append((first, base, parts))
        return first

    half_q = qdim // 2
    u_wo = add_seg(dim // WN, [(wo, 0, half_q), (wo, half_q, half_q)])
    u_gu = add_seg(ff // WN, [(wg, 0, dim), (wu, 0, dim)])
    u_dn = add_seg(dim // WN, [(wd, s, n) for s, n in chunks(ff)])
    u_wx = add_seg(inner // WN, [(wx, 0, dim)])
    u_wz = add_seg(inner // WN, [(wz, 0, dim)])
    u_out = add_seg(dim // WN, [(wout, s, n) for s, n in chunks(inner)])

    def copy(part, tile, slot):
        w, r0, nr = part
        return pltpu.make_async_copy(w.at[pl.ds(r0, nr), cols(tile)], ring.at[slot, pl.ds(0, nr)], ring_sem.at[slot])

    def start(u, lo, hi):
        for first, last, parts in segs:
            if hi < first or lo >= last:
                continue
            n = len(parts)
            for i, part in enumerate(parts):
                @pl.when((u >= first) & (u < last) & (lax.rem(u - first + n, n) == i))
                def _(part=part, first=first, n=n):
                    copy(part, lax.div(u - first, n), lax.rem(u, SLOTS)).start()

    def phase(first, n_tiles, body):
        parts = [s for s in segs if s[0] == first][0][2]
        n = len(parts)

        @pl.loop(0, n_tiles)
        def _(t):
            vals = []
            for i, part in enumerate(parts):
                slot = lax.rem(first + t * n + i, SLOTS)
                copy(part, 0, slot).wait()
                vals.append(ring.at[slot, pl.ds(0, part[2])])
            body(t, *vals)
            for i in range(n):
                start(first + t * n + i + SLOTS, first + SLOTS, first + SLOTS + n_tiles * n - 1)

    in_copies = [
        pltpu.make_async_copy(q_hbm, qo, in_sem.at[0]),
        pltpu.make_async_copy(k_hbm, kbuf, in_sem.at[1]),
        pltpu.make_async_copy(v_hbm, vbuf, in_sem.at[2]),
        pltpu.make_async_copy(x_hbm, h, in_sem.at[3]),
        pltpu.make_async_copy(wxp_hbm, wxp, in_sem.at[4]),
        pltpu.make_async_copy(wdt_hbm, wdt, in_sem.at[5]),
    ]
    for c in in_copies[:4]:
        c.start()
    for u in range(SLOTS):
        start(jnp.int32(u), u, u)
    for c in in_copies[4:]:
        c.start()
    for c in in_copies[:3]:
        c.wait()

    qi = lax.broadcasted_iota(jnp.int32, (seq, seq), 0)
    ki = lax.broadcasted_iota(jnp.int32, (seq, seq), 1)
    causal = jnp.concatenate([qi >= ki] * groups, axis=0)

    @pl.loop(0, kv_heads)
    def _(kvh):
        kcol = pl.ds(pl.multiple_of(kvh * 128, 128), 128)
        for b in range(n_seq):
            rs = pl.ds(b * seq, seq)
            kk = kbuf[rs, kcol]
            vv = vbuf[rs, kcol]
            qcols = [pl.ds(pl.multiple_of((kvh * groups + i) * 128, 128), 128) for i in range(groups)]
            qq = jnp.concatenate([qo[rs, c] for c in qcols], axis=0)
            s = lax.dot_general(qq, kk, (((1,), (1,)), ((), ())), preferred_element_type=F32) * 128 ** -0.5
            s = jnp.where(causal, s, -jnp.inf)
            e = jnp.exp(s - jnp.max(s, axis=-1, keepdims=True))
            p = (e * (1.0 / jnp.sum(e, axis=-1, keepdims=True))).astype(BF16)
            o = jnp.dot(p, vv, preferred_element_type=F32).astype(BF16)
            for i, c in enumerate(qcols):
                qo[rs, c] = o[i * seq:(i + 1) * seq]

    def norm_rows(g_idx):
        gain = norms[g_idx:g_idx + 1, :]

        @pl.loop(0, rows // 32)
        def _(i):
            rs = pl.ds(pl.multiple_of(i * 32, 32), 32)
            hv = h[rs, :].astype(F32)
            inv = lax.rsqrt(jnp.mean(hv * hv, axis=-1, keepdims=True) + EPS)
            a[rs, :] = (hv * inv * gain).astype(BF16)

    in_copies[3].wait()

    def wo_body(t, w0, w1):
        acc = jnp.dot(qo[:, :half_q], w0[...], preferred_element_type=F32)
        acc += jnp.dot(qo[:, half_q:], w1[...], preferred_element_type=F32)
        h[:, cols(t)] = (h[:, cols(t)].astype(F32) + acc).astype(BF16)

    phase(u_wo, dim // WN, wo_body)
    norm_rows(0)

    def gu_body(t, w0, w1):
        g = jnp.dot(a[...], w0[...], preferred_element_type=F32)
        u = jnp.dot(a[...], w1[...], preferred_element_type=F32)
        act[:, cols(t)] = (silu(g) * u).astype(BF16)

    phase(u_gu, ff // WN, gu_body)

    def dn_body(t, *ws):
        acc = None
        for (s, n), w in zip(chunks(ff), ws):
            d = jnp.dot(act[:, s:s + n], w[...], preferred_element_type=F32)
            acc = d if acc is None else acc + d
        h[:, cols(t)] = (h[:, cols(t)].astype(F32) + acc).astype(BF16)

    phase(u_dn, dim // WN, dn_body)
    norm_rows(1)

    row_id = lax.broadcasted_iota(jnp.int32, (seq, 1), 0)

    def scatter(dst, r0, t, val):
        for j in range(WN // 128):
            for i in range(seq // 8):
                dst[pl.ds((r0 + i * 8) * PITCH + t * (WN // 128) + j, 8, stride=PITCH), :] = (
                    val[i * 8:(i + 1) * 8, j * 128:(j + 1) * 128])

    def wx_body(t, w):
        res = jnp.dot(a[...], w[...], preferred_element_type=F32).astype(BF16).astype(F32)
        for b in range(n_seq):
            xi = res[b * seq:(b + 1) * seq]
            acc = chan[4:5, cols(t)] + chan[CONV - 1:CONV, cols(t)] * xi
            for j in range(CONV - 1):
                back = CONV - 1 - j
                prev = jnp.where(row_id >= back, pltpu.roll(xi, back, axis=0), 0.0)
                acc += chan[j:j + 1, cols(t)] * prev
            c = silu(acc).astype(BF16)
            xc[b * seq:(b + 1) * seq, cols(t)] = c
            scatter(xs, b * seq, t, c.astype(F32))

    phase(u_wx, inner // WN, wx_body)

    def wz_body(t, w):
        zg[:, cols(t)] = jnp.dot(a[...], w[...], preferred_element_type=F32).astype(BF16)

    phase(u_wz, inner // WN, wz_body)

    in_copies[4].wait()
    r = lax.dot_general(xc[...], wxp[...], (((1,), (1,)), ((), ())), preferred_element_type=F32)
    n_r = r.shape[1]
    col = lax.broadcasted_iota(jnp.int32, (1, n_r), 1)
    sq = r * r

    def inv_of(mask, n):
        return lax.rsqrt(jnp.sum(jnp.where(mask, sq, 0.0), axis=-1, keepdims=True) * (1.0 / n) + EPS)

    m_dt = col < dt_rank
    m_b = (col >= dt_rank) & (col < dt_rank + n_state)
    m_c = col >= dt_rank + n_state
    inv = jnp.where(m_dt, inv_of(m_dt, dt_rank), jnp.where(m_b, inv_of(m_b, n_state), inv_of(m_c, n_state)))
    rn = r * inv * gains[0:1, :]
    for n in range(n_state):
        bb[n * rows:(n + 1) * rows, :] = jnp.broadcast_to(rn[:, dt_rank + n:dt_rank + n + 1], (rows, 128))
        c0 = dt_rank + n_state + n
        cb[n * rows:(n + 1) * rows, :] = jnp.broadcast_to(rn[:, c0:c0 + 1], (rows, 128))
    dt_in = rn[:, :dt_rank].astype(BF16)
    a[:, :dt_rank] = dt_in
    in_copies[5].wait()

    @pl.loop(0, inner // WN)
    def _(t):
        pre = jnp.dot(a[:, :dt_rank], wdt[:, cols(t)], preferred_element_type=F32) + chan[5:6, cols(t)]
        step = jnp.maximum(pre, 0.0) + jnp.log1p(jnp.exp(-jnp.abs(pre)))
        for b in range(n_seq):
            scatter(delta, b * seq, t, step[b * seq:(b + 1) * seq])

    def bcast(ref, idx):
        return jnp.broadcast_to(ref[pl.ds(idx, 1), :], (8, 128))

    @pl.loop(0, n_seq)
    def _(b):
        @pl.loop(0, lanes // 8)
        def _(c):
            av = [a2[pl.ds(pl.multiple_of(n * lanes + c * 8, 8), 8), :] for n in range(n_state)]
            dsk = dskip[pl.ds(pl.multiple_of(c * 8, 8), 8), :]

            def step(i, st):
                st = list(st)
                for k in range(4):
                    r = b * seq + i * 4 + k
                    at = pl.ds(r * PITCH + c * 8, 8)
                    d = delta[at, :]
                    x = xs[at, :]
                    dx = d * x
                    terms = []
                    for n in range(n_state):
                        st[n] = jnp.exp2(d * av[n]) * st[n] + dx * bcast(bb, n * rows + r)
                        terms.append(st[n] * bcast(cb, n * rows + r))
                    terms.append(dsk * x)
                    while len(terms) > 1:
                        terms = [terms[m] + terms[m + 1] for m in range(0, len(terms) - 1, 2)] + (
                            [terms[-1]] if len(terms) % 2 else [])
                    delta[at, :] = terms[0]
                return tuple(st)

            lax.fori_loop(0, seq // 4, step, tuple(jnp.zeros((8, 128), F32) for _ in range(n_state)))

    @pl.loop(0, rows // 16)
    def _(i):
        r0 = pl.multiple_of(i * 16, 16)
        for j in range(lanes):
            y = jnp.concatenate([delta[pl.ds((r0 + 8 * m) * PITCH + j, 8, stride=PITCH), :] for m in range(2)], axis=0)
            z = zg[pl.ds(r0, 16), j * 128:(j + 1) * 128].astype(F32)
            act[pl.ds(r0, 16), j * 128:(j + 1) * 128] = (y * silu(z)).astype(BF16)

    def out_body(t, *ws):
        acc = None
        for (s, n), w in zip(chunks(inner), ws):
            d = jnp.dot(act[:, s:s + n], w[...], preferred_element_type=F32)
            acc = d if acc is None else acc + d
        out_ref[:, cols(t)] = (h[:, cols(t)].astype(F32) + acc).astype(BF16)

    phase(u_out, dim // WN, out_body)


def layer_pair(hidden, attn_norm, w_q, w_k, w_v, w_o, mlp_norm, w_gate, w_up, w_down, mamba_norm, w_in_x, w_in_z, conv_w, conv_b, w_xproj, dt_norm, b_norm, c_norm, w_dt, dt_bias, a_log, d_skip, w_out):
    dim = hidden.shape[-1]
    x = lax.all_to_all(hidden, "sp", 0, 1, tiled=True)
    n_seq, seq, _ = x.shape
    rows = n_seq * seq
    x = x.reshape(rows, dim)
    inner, n_state = a_log.shape
    normed = rms_scale(x, attn_norm).astype(BF16)

    def proj(w):
        return jnp.einsum("rd,dhk->rhk", normed, w, preferred_element_type=F32).astype(BF16).reshape(rows, -1)

    q, k, v = proj(w_q), proj(w_k), proj(w_v)
    lanes = inner // 128
    norms = jnp.stack([mlp_norm, mamba_norm]).astype(F32)
    chan = jnp.concatenate([conv_w.astype(F32), conv_b.astype(F32)[None], dt_bias[None], jnp.zeros((2, inner), F32)])
    gains = jnp.concatenate([dt_norm, b_norm, c_norm])[None]
    a2 = (-jnp.exp(a_log.T) * LOG2E).reshape(n_state * lanes, 128)
    dskip = d_skip.reshape(lanes, 128)
    hbm = pl.BlockSpec(memory_space=pltpu.HBM)
    vm = pl.BlockSpec(memory_space=pltpu.VMEM)
    out = pl.pallas_call(
        block_kernel,
        out_shape=jax.ShapeDtypeStruct((rows, dim), BF16),
        in_specs=[hbm] * 13 + [vm] * 5,
        out_specs=vm,
        scratch_shapes=[
            pltpu.VMEM((SLOTS, dim, WN), BF16),
            pltpu.VMEM(q.shape, BF16),
            pltpu.VMEM(k.shape, BF16),
            pltpu.VMEM(v.shape, BF16),
            pltpu.VMEM((rows, dim), BF16),
            pltpu.VMEM((rows, dim), BF16),
            pltpu.VMEM((rows, w_gate.shape[1]), BF16),
            pltpu.VMEM((rows, inner), BF16),
            pltpu.VMEM((rows, inner), BF16),
            pltpu.VMEM((rows * PITCH, 128), F32),
            pltpu.VMEM((rows * PITCH, 128), F32),
            pltpu.VMEM((rows * n_state, 128), F32),
            pltpu.VMEM((rows * n_state, 128), F32),
            pltpu.VMEM((w_xproj.shape[1], inner), BF16),
            pltpu.VMEM(w_dt.shape, BF16),
            pltpu.SemaphoreType.DMA((SLOTS,)),
            pltpu.SemaphoreType.DMA((6,)),
        ],
        compiler_params=pltpu.CompilerParams(vmem_limit_bytes=67043328),
        name="block",
    )(q, k, v, x, w_o.reshape(-1, dim), w_gate, w_up, w_down, w_in_x, w_in_z, w_xproj.T, w_dt, w_out,
      norms, chan, gains, dskip, a2)
    return lax.all_to_all(out.reshape(n_seq, seq, dim), "sp", 1, 0, tiled=True)


def solution(mesh):
    act_spec = P("dp", "sp", None)
    return jax.shard_map(
        layer_pair,
        mesh=mesh,
        in_specs=(act_spec,) + (P(),) * 23,
        out_specs=act_spec,
        check_vma=False,
    )
```

```python
import functools
import math
import jax
import jax.numpy as jnp
from jax import lax
from jax.experimental import pallas as pl
from jax.experimental.pallas import tpu as pltpu
from jax.sharding import PartitionSpec as P

EPS = 1e-6
CONV = 4
SLOTS = 12
STAGE = 4
KB = 64
WN = 512
PITCH = 41
F32 = jnp.float32
BF16 = jnp.bfloat16
LOG2E = math.log2(math.e)


def rms_scale(values, gain_vec):
    values_f = values.astype(F32)
    inv_rms = lax.rsqrt(jnp.mean(values_f * values_f, axis=-1, keepdims=True) + EPS)
    return values_f * inv_rms * gain_vec.astype(F32)


def silu(v):
    half = 0.5 * v
    return half + half * jnp.tanh(half)


def block_kernel(x_hbm, wq, wk, wv, wo, wg, wu, wd, wx, wz, wxp_hbm, wdt_hbm, wout,
                 norms, chan, gains, dskip, a2, out_ref,
                 ring, stage, tmp, qkv, h, a, act, delta, xs, bb, cb, wxp, wdt,
                 ring_sem, stage_sem, in_sem, send_sem, recv_sem):
    rows, dim = h.shape
    n_seq, seq = 2, 128
    n_dev = x_hbm.shape[0] // n_seq
    tok = x_hbm.shape[1]
    me = lax.axis_index("sp")
    inner = wx.shape[1]
    ff = wg.shape[1]
    qdim = wo.shape[0]
    heads = qdim // 128
    kv_heads = (qkv.shape[1] - qdim) // 256
    groups = heads // kv_heads
    lanes = inner // 128
    n_state = a2.shape[0] // lanes
    dt_rank = wdt.shape[0]
    unit = ring.shape[1]

    def chunks(total):
        return [(s, min(unit, total - s)) for s in range(0, total, unit)]

    def cols(t):
        return pl.ds(pl.multiple_of(t * WN, WN), WN)

    segs = []
    base = 0

    def add_seg(n_tiles, parts):
        nonlocal base
        first = base
        base = first + n_tiles * len(parts)
        segs.append((first, base, parts))
        return first

    half_q = qdim // 2
    u_qkv = add_seg(qkv.shape[1] // WN, [(None, 0, dim)])
    u_wo = add_seg(dim // WN, [(wo, 0, half_q), (wo, half_q, half_q)])
    u_gu = add_seg(ff // WN, [(wg, 0, dim), (wu, 0, dim)])
    u_dn = add_seg(dim // WN, [(wd, s, n) for s, n in chunks(ff)])
    u_wx = add_seg(inner // WN, [(wx, 0, dim)])
    u_wz = add_seg(inner // WN, [(wz, 0, dim)])
    u_out = add_seg(dim // WN, [(wout, s, n) for s, n in chunks(inner)])

    def copy(part, tile, slot):
        w, r0, nr = part
        return pltpu.make_async_copy(w.at[pl.ds(r0, nr), cols(tile)], ring.at[slot, pl.ds(0, nr)], ring_sem.at[slot])

    def start(u, lo, hi):
        for first, last, parts in segs:
            if hi < first or lo >= last or parts[0][0] is None:
                continue
            n = len(parts)
            for i, part in enumerate(parts):
                @pl.when((u >= first) & (u < last) & (lax.rem(u - first + n, n) == i))
                def _(part=part, first=first, n=n):
                    copy(part, lax.div(u - first, n), lax.rem(u, SLOTS)).start()

    def phase(first, n_tiles, body):
        parts = [s for s in segs if s[0] == first][0][2]
        n = len(parts)

        @pl.loop(0, n_tiles)
        def _(t):
            vals = []
            for i, part in enumerate(parts):
                slot = lax.rem(first + t * n + i, SLOTS)
                if part[0] is not None:
                    copy(part, 0, slot).wait()
                vals.append(ring.at[slot, pl.ds(0, part[2])])
            body(t, *vals)
            for i in range(n):
                start(first + t * n + i + SLOTS, first + SLOTS, first + SLOTS + n_tiles * n - 1)

    def norm_rows(g_idx):
        gain = norms[g_idx:g_idx + 1, :]

        @pl.loop(0, rows // 32)
        def _(i):
            rs = pl.ds(pl.multiple_of(i * 32, 32), 32)
            hv = h[rs, :].astype(F32)
            inv = lax.rsqrt(jnp.mean(hv * hv, axis=-1, keepdims=True) + EPS)
            a[rs, :] = (hv * inv * gain).astype(BF16)

    in_copies = [
        pltpu.make_async_copy(wxp_hbm, wxp, in_sem.at[0]),
        pltpu.make_async_copy(wdt_hbm, wdt, in_sem.at[1]),
    ]
    n_q = wq.shape[0] // KB
    n_kv = wk.shape[0] // KB

    def stage_copy(w, c, slot):
        return pltpu.make_async_copy(w.at[pl.ds(c * KB, KB)], stage.at[slot], stage_sem.at[slot])

    def stage_start(i):
        slot = lax.rem(i, STAGE)
        for w, lo, n in ((wq, 0, n_q), (wk, n_q, n_kv), (wv, n_q + n_kv, n_kv)):
            @pl.when((i >= lo) & (i < lo + n))
            def _(w=w, lo=lo):
                stage_copy(w, i - lo, slot).start()

    for i in range(STAGE):
        stage_start(jnp.int32(i))

    barrier = pltpu.get_barrier_semaphore()
    for d in range(1, n_dev):
        pl.semaphore_signal(barrier, inc=1, device_id={"sp": lax.rem(me + d, n_dev)}, device_id_type=pl.DeviceIdType.MESH)
    pl.semaphore_wait(barrier, n_dev - 1)

    def exchange(src_of, dst_of, ex):
        for d in range(1, n_dev):
            peer = lax.rem(me + d, n_dev)
            for b in range(n_seq):
                pltpu.make_async_remote_copy(
                    src_ref=src_of(peer, b), dst_ref=dst_of(me, b), send_sem=send_sem.at[ex], recv_sem=recv_sem.at[ex],
                    device_id={"sp": peer}, device_id_type=pl.DeviceIdType.MESH).start()
        for b in range(n_seq):
            pltpu.make_async_copy(src_of(me, b), dst_of(me, b), recv_sem.at[ex]).start()

    def exchange_wait(whole_dst, part_src, ex):
        pltpu.make_async_copy(whole_dst, whole_dst, recv_sem.at[ex]).wait()
        pltpu.make_async_copy(part_src, part_src, send_sem.at[ex]).wait()

    def blk(owner, b):
        return pl.ds(pl.multiple_of(b * seq + owner * tok, tok), tok)

    exchange(lambda p, b: x_hbm.at[p * n_seq + b], lambda p, b: h.at[blk(p, b)], 0)
    for c in in_copies:
        c.start()

    def relayout(i, n_heads, unit0, k0):
        slot = lax.rem(i, STAGE)
        per = 32 // n_heads
        pitch = n_heads + 1
        stage_copy(wq, 0, slot).wait()

        @pl.loop(0, KB * per // 16)
        def _(g):
            buf = tmp.at[lax.rem(g, 2)]
            for r in range(16 // per):
                val = stage[slot, g * (16 // per) + r].astype(F32)
                for j in range(per):
                    buf[pl.ds((r * per + j) * pitch, n_heads), :] = val[j * n_heads:(j + 1) * n_heads]
            ks = pl.ds(pl.multiple_of(k0 + g * 16, 16), 16)
            for hd in range(n_heads):
                w = WN // 128
                ring[unit0 + hd // w, ks, (hd % w) * 128:(hd % w + 1) * 128] = (
                    buf[pl.ds(hd, 16, stride=pitch), :].astype(BF16))

        stage_start(i + STAGE)

    @pl.loop(0, n_q)
    def _(i):
        relayout(i, heads, 0, i * KB)

    for m in range(2):
        @pl.loop(0, n_kv)
        def _(i, m=m):
            relayout(n_q + m * n_kv + i, kv_heads, (qdim + m * kv_heads * 128) // WN, i * KB * (32 // kv_heads))

    exchange_wait(h, h.at[pl.ds(0, rows - n_seq * tok)], 0)
    norm_rows(0)

    def qkv_body(t, w):
        qkv[:, cols(t)] = jnp.dot(a[...], w[...], preferred_element_type=F32).astype(BF16)

    phase(u_qkv, qkv.shape[1] // WN, qkv_body)

    qi = lax.broadcasted_iota(jnp.int32, (seq, seq), 0)
    ki = lax.broadcasted_iota(jnp.int32, (seq, seq), 1)
    causal = jnp.concatenate([qi >= ki] * groups, axis=0)

    @pl.loop(0, kv_heads)
    def _(kvh):
        for b in range(n_seq):
            rs = pl.ds(b * seq, seq)
            kk = qkv[rs, pl.ds(pl.multiple_of(qdim + kvh * 128, 128), 128)]
            vv = qkv[rs, pl.ds(pl.multiple_of(qdim + (kv_heads + kvh) * 128, 128), 128)]
            qcols = [pl.ds(pl.multiple_of((kvh * groups + i) * 128, 128), 128) for i in range(groups)]
            qq = jnp.concatenate([qkv[rs, c] for c in qcols], axis=0)
            s = lax.dot_general(qq, kk, (((1,), (1,)), ((), ())), preferred_element_type=F32) * 128 ** -0.5
            s = jnp.where(causal, s, -jnp.inf)
            e = jnp.exp(s - jnp.max(s, axis=-1, keepdims=True))
            p = (e * (1.0 / jnp.sum(e, axis=-1, keepdims=True))).astype(BF16)
            o = jnp.dot(p, vv, preferred_element_type=F32).astype(BF16)
            for i, c in enumerate(qcols):
                qkv[rs, c] = o[i * seq:(i + 1) * seq]

    def wo_body(t, w0, w1):
        acc = jnp.dot(qkv[:, :half_q], w0[...], preferred_element_type=F32)
        acc += jnp.dot(qkv[:, half_q:qdim], w1[...], preferred_element_type=F32)
        h[:, cols(t)] = (h[:, cols(t)].astype(F32) + acc).astype(BF16)

    phase(u_wo, dim // WN, wo_body)
    norm_rows(1)

    def gu_body(t, w0, w1):
        g = jnp.dot(a[...], w0[...], preferred_element_type=F32)
        u = jnp.dot(a[...], w1[...], preferred_element_type=F32)
        act[:, cols(t)] = (silu(g) * u).astype(BF16)

    phase(u_gu, ff // WN, gu_body)

    def dn_body(t, *ws):
        acc = None
        for (s, n), w in zip(chunks(ff), ws):
            d = jnp.dot(act[:, s:s + n], w[...], preferred_element_type=F32)
            acc = d if acc is None else acc + d
        h[:, cols(t)] = (h[:, cols(t)].astype(F32) + acc).astype(BF16)

    phase(u_dn, dim // WN, dn_body)
    norm_rows(2)

    row_id = lax.broadcasted_iota(jnp.int32, (seq, 1), 0)

    def scatter(dst, r0, t, val):
        for j in range(WN // 128):
            for i in range(seq // 8):
                dst[pl.ds((r0 + i * 8) * PITCH + t * (WN // 128) + j, 8, stride=PITCH), :] = (
                    val[i * 8:(i + 1) * 8, j * 128:(j + 1) * 128])

    def wx_body(t, w):
        res = jnp.dot(a[...], w[...], preferred_element_type=F32).astype(BF16).astype(F32)
        for b in range(n_seq):
            xi = res[b * seq:(b + 1) * seq]
            acc = chan[4:5, cols(t)] + chan[CONV - 1:CONV, cols(t)] * xi
            for j in range(CONV - 1):
                back = CONV - 1 - j
                prev = jnp.where(row_id >= back, pltpu.roll(xi, back, axis=0), 0.0)
                acc += chan[j:j + 1, cols(t)] * prev
            c = silu(acc).astype(BF16)
            act[b * seq:(b + 1) * seq, cols(t)] = c
            scatter(xs, b * seq, t, c.astype(F32))

    phase(u_wx, inner // WN, wx_body)

    def wz_body(t, w):
        qkv[:, cols(t)] = jnp.dot(a[...], w[...], preferred_element_type=F32).astype(BF16)

    phase(u_wz, inner // WN, wz_body)

    in_copies[0].wait()
    r = lax.dot_general(act[:, :inner], wxp[...], (((1,), (1,)), ((), ())), preferred_element_type=F32)
    n_r = r.shape[1]
    col = lax.broadcasted_iota(jnp.int32, (1, n_r), 1)
    sq = r * r

    def inv_of(mask, n):
        return lax.rsqrt(jnp.sum(jnp.where(mask, sq, 0.0), axis=-1, keepdims=True) * (1.0 / n) + EPS)

    m_dt = col < dt_rank
    m_b = (col >= dt_rank) & (col < dt_rank + n_state)
    m_c = col >= dt_rank + n_state
    inv = jnp.where(m_dt, inv_of(m_dt, dt_rank), jnp.where(m_b, inv_of(m_b, n_state), inv_of(m_c, n_state)))
    rn = r * inv * gains[0:1, :]
    for n in range(n_state):
        bb[n * rows:(n + 1) * rows, :] = jnp.broadcast_to(rn[:, dt_rank + n:dt_rank + n + 1], (rows, 128))
        c0 = dt_rank + n_state + n
        cb[n * rows:(n + 1) * rows, :] = jnp.broadcast_to(rn[:, c0:c0 + 1], (rows, 128))
    dt_in = rn[:, :dt_rank].astype(BF16)
    a[:, :dt_rank] = dt_in
    in_copies[1].wait()

    @pl.loop(0, inner // WN)
    def _(t):
        pre = jnp.dot(a[:, :dt_rank], wdt[:, cols(t)], preferred_element_type=F32) + chan[5:6, cols(t)]
        step = jnp.maximum(pre, 0.0) + jnp.log1p(jnp.exp(-jnp.abs(pre)))
        for b in range(n_seq):
            scatter(delta, b * seq, t, step[b * seq:(b + 1) * seq])

    def bcast(ref, idx):
        return jnp.broadcast_to(ref[pl.ds(idx, 1), :], (8, 128))

    @pl.loop(0, n_seq)
    def _(b):
        @pl.loop(0, lanes // 8)
        def _(c):
            av = [a2[pl.ds(pl.multiple_of(n * lanes + c * 8, 8), 8), :] for n in range(n_state)]
            dsk = dskip[pl.ds(pl.multiple_of(c * 8, 8), 8), :]

            def step(i, st):
                st = list(st)
                for k in range(4):
                    r = b * seq + i * 4 + k
                    at = pl.ds(r * PITCH + c * 8, 8)
                    d = delta[at, :]
                    x = xs[at, :]
                    dx = d * x
                    terms = []
                    for n in range(n_state):
                        st[n] = jnp.exp2(d * av[n]) * st[n] + dx * bcast(bb, n * rows + r)
                        terms.append(st[n] * bcast(cb, n * rows + r))
                    terms.append(dsk * x)
                    while len(terms) > 1:
                        terms = [terms[m] + terms[m + 1] for m in range(0, len(terms) - 1, 2)] + (
                            [terms[-1]] if len(terms) % 2 else [])
                    delta[at, :] = terms[0]
                return tuple(st)

            lax.fori_loop(0, seq // 4, step, tuple(jnp.zeros((8, 128), F32) for _ in range(n_state)))

    @pl.loop(0, rows // 16)
    def _(i):
        r0 = pl.multiple_of(i * 16, 16)
        for j in range(lanes):
            y = jnp.concatenate([delta[pl.ds((r0 + 8 * m) * PITCH + j, 8, stride=PITCH), :] for m in range(2)], axis=0)
            z = qkv[pl.ds(r0, 16), j * 128:(j + 1) * 128].astype(F32)
            act[pl.ds(r0, 16), j * 128:(j + 1) * 128] = (y * silu(z)).astype(BF16)

    def out_body(t, *ws):
        acc = None
        for (s, n), w in zip(chunks(inner), ws):
            d = jnp.dot(act[:, s:s + n], w[...], preferred_element_type=F32)
            acc = d if acc is None else acc + d
        a[:, cols(t)] = (h[:, cols(t)].astype(F32) + acc).astype(BF16)
        exchange(lambda p, b: a.at[blk(p, b), cols(t)], lambda p, b: out_ref.at[p * n_seq + b, :, cols(t)], 1)

    phase(u_out, dim // WN, out_body)
    exchange_wait(out_ref, a.at[pl.ds(0, rows - n_seq * tok)], 1)


def layer_pair(hidden, attn_norm, w_q, w_k, w_v, w_o, mlp_norm, w_gate, w_up, w_down, mamba_norm, w_in_x, w_in_z, conv_w, conv_b, w_xproj, dt_norm, b_norm, c_norm, w_dt, dt_bias, a_log, d_skip, w_out):
    n_batch, tok, dim = hidden.shape
    n_seq = n_batch // lax.axis_size("sp")
    rows = n_batch * tok
    inner, n_state = a_log.shape
    lanes = inner // 128
    norms = jnp.stack([attn_norm, mlp_norm, mamba_norm]).astype(F32)
    chan = jnp.concatenate([conv_w.astype(F32), conv_b.astype(F32)[None], dt_bias[None], jnp.zeros((2, inner), F32)])
    gains = jnp.concatenate([dt_norm, b_norm, c_norm])[None]
    a2 = (-jnp.exp(a_log.T) * LOG2E).reshape(n_state * lanes, 128)
    dskip = d_skip.reshape(lanes, 128)
    hbm = pl.BlockSpec(memory_space=pltpu.HBM)
    vm = pl.BlockSpec(memory_space=pltpu.VMEM)
    qkv_dim = (w_q.shape[1] + w_k.shape[1] + w_v.shape[1]) * 128
    return pl.pallas_call(
        block_kernel,
        out_shape=jax.ShapeDtypeStruct(hidden.shape, BF16),
        in_specs=[hbm] * 13 + [vm] * 5,
        out_specs=hbm,
        scratch_shapes=[
            pltpu.VMEM((SLOTS, dim, WN), BF16),
            pltpu.VMEM((STAGE, KB, 32, 128), BF16),
            pltpu.VMEM((2, 16 * 33, 128), F32),
            pltpu.VMEM((rows, qkv_dim), BF16),
            pltpu.VMEM((rows, dim), BF16),
            pltpu.VMEM((rows, dim), BF16),
            pltpu.VMEM((rows, w_gate.shape[1]), BF16),
            pltpu.VMEM((rows * PITCH, 128), F32),
            pltpu.VMEM((rows * PITCH, 128), F32),
            pltpu.VMEM((rows * n_state, 128), F32),
            pltpu.VMEM((rows * n_state, 128), F32),
            pltpu.VMEM((w_xproj.shape[1], inner), BF16),
            pltpu.VMEM(w_dt.shape, BF16),
            pltpu.SemaphoreType.DMA((SLOTS,)),
            pltpu.SemaphoreType.DMA((STAGE,)),
            pltpu.SemaphoreType.DMA((2,)),
            pltpu.SemaphoreType.DMA((2,)),
            pltpu.SemaphoreType.DMA((2,)),
        ],
        compiler_params=pltpu.CompilerParams(vmem_limit_bytes=67043328, collective_id=0, has_side_effects=True),
        name="block",
    )(hidden, w_q.reshape(-1, 32, 128), w_k.reshape(-1, 32, 128), w_v.reshape(-1, 32, 128), w_o.reshape(-1, dim),
      w_gate, w_up, w_down, w_in_x, w_in_z, w_xproj.T, w_dt, w_out, norms, chan, gains, dskip, a2)


def solution(mesh):
    act_spec = P("dp", "sp", None)
    return jax.shard_map(
        layer_pair,
        mesh=mesh,
        in_specs=(act_spec,) + (P(),) * 23,
        out_specs=act_spec,
        check_vma=False,
    )
```

```python
import functools
import math
import jax
import jax.numpy as jnp
from jax import lax
from jax.experimental import pallas as pl
from jax.experimental.pallas import tpu as pltpu
from jax.sharding import PartitionSpec as P

EPS = 1e-6
CONV = 4
SLOTS = 12
STAGE = 6
KB = 64
WN = 512
PITCH = 41
F32 = jnp.float32
BF16 = jnp.bfloat16
LOG2E = math.log2(math.e)


def rms_scale(values, gain_vec):
    values_f = values.astype(F32)
    inv_rms = lax.rsqrt(jnp.mean(values_f * values_f, axis=-1, keepdims=True) + EPS)
    return values_f * inv_rms * gain_vec.astype(F32)


def silu(v):
    half = 0.5 * v
    return half + half * jnp.tanh(half)


def block_kernel(x_hbm, wq, wk, wv, wo, wg, wu, wd, wx, wz, wxp_hbm, wdt_hbm, wout,
                 attn_g, mlp_g, mamba_g, conv_w, conv_b, dt_g, b_g, c_g, dt_b, dskip, a_log, out_ref,
                 ring, stage, acc_ref, qkv, h, a, act, delta, xs, bb, cb, wxp, wdt, a2, chan, rn_ref,
                 ring_sem, stage_sem, in_sem, send_sem, recv_sem):
    rows, dim = h.shape
    n_seq, seq = 2, 128
    n_dev = x_hbm.shape[0] // n_seq
    tok = x_hbm.shape[1]
    me = lax.axis_index("sp")
    inner = wx.shape[1]
    ff = wg.shape[1]
    qdim = wo.shape[0]
    heads = qdim // 128
    kv_heads = (qkv.shape[1] - qdim) // 256
    groups = heads // kv_heads
    lanes = inner // 128
    n_state = a_log.shape[0]
    dt_rank = wdt.shape[0]
    unit = ring.shape[1]

    def chunks(total):
        return [(s, min(unit, total - s)) for s in range(0, total, unit)]

    def cols(t):
        return pl.ds(pl.multiple_of(t * WN, WN), WN)

    segs = []
    base = 0

    def add_seg(n_tiles, parts):
        nonlocal base
        first = base
        base = first + n_tiles * len(parts)
        segs.append((first, base, parts))
        return first

    half_q = qdim // 2
    u_qkv = add_seg(qkv.shape[1] // WN, [(None, 0, dim)])
    u_wo = add_seg(dim // WN, [(wo, 0, half_q), (wo, half_q, half_q)])
    u_gu = add_seg(ff // WN, [(wg, 0, dim), (wu, 0, dim)])
    u_dn = add_seg(dim // WN, [(wd, s, n) for s, n in chunks(ff)])
    u_wx = add_seg(inner // WN, [(wx, 0, dim)])
    u_wz = add_seg(inner // WN, [(wz, 0, dim)])
    u_out = add_seg(dim // WN, [(wout, s, n) for s, n in chunks(inner)])

    def copy(part, tile, slot):
        w, r0, nr = part
        return pltpu.make_async_copy(w.at[pl.ds(r0, nr), cols(tile)], ring.at[slot, pl.ds(0, nr)], ring_sem.at[slot])

    def start(u, lo, hi):
        for first, last, parts in segs:
            if hi < first or lo >= last or parts[0][0] is None:
                continue
            n = len(parts)
            for i, part in enumerate(parts):
                @pl.when((u >= first) & (u < last) & (lax.rem(u - first + n, n) == i))
                def _(part=part, first=first, n=n):
                    copy(part, lax.div(u - first, n), lax.rem(u, SLOTS)).start()

    def phase(first, n_tiles, body, per=1):
        parts = [s for s in segs if s[0] == first][0][2]
        n = len(parts)

        def group(t0, count):
            views = []
            for u in range(count * n):
                slot = lax.rem(first + t0 * n + u, SLOTS)
                part = parts[u % n]
                if part[0] is not None:
                    copy(part, 0, slot).wait()
                views.append(ring.at[slot, pl.ds(0, part[2])])
            for m in range(count):
                body(t0 + m, *views[m * n:(m + 1) * n])
            for u in range(count * n):
                start(first + t0 * n + u + SLOTS, first + SLOTS, first + SLOTS + n_tiles * n - 1)

        @pl.loop(0, n_tiles // per)
        def _(g):
            group(g * per, per)

        if n_tiles % per:
            group(jnp.int32(n_tiles - n_tiles % per), n_tiles % per)

    def norm_rows(g_ref):
        gain = g_ref[...].astype(F32).reshape(1, dim)

        @pl.loop(0, rows // 32)
        def _(i):
            rs = pl.ds(pl.multiple_of(i * 32, 32), 32)
            hv = h[rs, :].astype(F32)
            inv = lax.rsqrt(jnp.mean(hv * hv, axis=-1, keepdims=True) + EPS)
            a[rs, :] = (hv * inv * gain).astype(BF16)

    in_copies = [
        pltpu.make_async_copy(wxp_hbm, wxp, in_sem.at[0]),
        pltpu.make_async_copy(wdt_hbm, wdt, in_sem.at[1]),
    ]
    n_q = wq.shape[0] // KB
    n_kv = wk.shape[0] // KB

    def stage_copy(w, c, slot):
        return pltpu.make_async_copy(w.at[pl.ds(c * KB, KB)], stage.at[slot], stage_sem.at[slot])

    def stage_start(i):
        slot = lax.rem(i, STAGE)
        for w, lo, n in ((wq, 0, n_q), (wk, n_q, n_kv), (wv, n_q + n_kv, n_kv)):
            @pl.when((i >= lo) & (i < lo + n))
            def _(w=w, lo=lo):
                stage_copy(w, i - lo, slot).start()

    for i in range(STAGE):
        stage_start(jnp.int32(i))

    barrier = pltpu.get_barrier_semaphore()
    for d in range(1, n_dev):
        pl.semaphore_signal(barrier, inc=1, device_id={"sp": lax.rem(me + d, n_dev)}, device_id_type=pl.DeviceIdType.MESH)
    pl.semaphore_wait(barrier, n_dev - 1)

    def exchange(src_of, dst_of, ex, bs):
        for d in range(1, n_dev):
            peer = lax.rem(me + d, n_dev)
            for b in bs:
                pltpu.make_async_remote_copy(
                    src_ref=src_of(peer, b), dst_ref=dst_of(me, b), send_sem=send_sem.at[ex], recv_sem=recv_sem.at[ex],
                    device_id={"sp": peer}, device_id_type=pl.DeviceIdType.MESH).start()
        for b in bs:
            pltpu.make_async_copy(src_of(me, b), dst_of(me, b), recv_sem.at[ex]).start()

    def exchange_wait(whole_dst, part_src, ex):
        pltpu.make_async_copy(whole_dst, whole_dst, recv_sem.at[ex]).wait()
        pltpu.make_async_copy(part_src, part_src, send_sem.at[ex]).wait()

    def blk(owner, b):
        return pl.ds(pl.multiple_of(b * seq + owner * tok, tok), tok)

    exchange(lambda p, b: x_hbm.at[p * n_seq + b], lambda p, b: h.at[blk(p, b)], 0, range(n_seq))
    for c in in_copies:
        c.start()

    chan[0:CONV, :] = conv_w[...].astype(F32)
    chan[CONV:CONV + 1, :] = conv_b[...].astype(F32).reshape(1, inner)
    chan[CONV + 1:CONV + 2, :] = dt_b[...].reshape(1, inner)
    for j in range(lanes):
        neg = -jnp.exp(a_log[:, j * 128:(j + 1) * 128]) * LOG2E
        for m in range(n_state // 8):
            a2[pl.ds(m * 8 * PITCH + j, 8, stride=PITCH), :] = neg[m * 8:(m + 1) * 8]

    def relayout(i, n_heads, unit0, k0):
        slot = lax.rem(i, STAGE)
        per = 32 // n_heads
        pitch = n_heads + 1
        stage_copy(wq, 0, slot).wait()

        @pl.loop(0, KB * per // 32)
        def _(g2):
            for m in range(2):
                g = g2 * 2 + m
                base_row = m * 16 * 33
                for r in range(16 // per):
                    val = stage[slot, g * (16 // per) + r].astype(F32)
                    for j in range(per):
                        delta[pl.ds(base_row + (r * per + j) * pitch, n_heads), :] = val[j * n_heads:(j + 1) * n_heads]
                ks = pl.ds(pl.multiple_of(k0 + g * 16, 16), 16)
                for hd in range(n_heads):
                    w = WN // 128
                    ring[unit0 + hd // w, ks, (hd % w) * 128:(hd % w + 1) * 128] = (
                        delta[pl.ds(base_row + hd, 16, stride=pitch), :].astype(BF16))

        stage_start(i + STAGE)

    @pl.loop(0, n_q)
    def _(i):
        relayout(i, heads, 0, i * KB)

    for m in range(2):
        @pl.loop(0, n_kv)
        def _(i, m=m):
            relayout(n_q + m * n_kv + i, kv_heads, (qdim + m * kv_heads * 128) // WN, i * KB * (32 // kv_heads))

    exchange_wait(h, h.at[pl.ds(0, rows - n_seq * tok)], 0)
    norm_rows(attn_g)

    def qkv_body(t, w):
        qkv[:, cols(t)] = jnp.dot(a[...], w[...], preferred_element_type=F32).astype(BF16)

    phase(u_qkv, qkv.shape[1] // WN, qkv_body, 3)

    qi = lax.broadcasted_iota(jnp.int32, (seq, seq), 0)
    ki = lax.broadcasted_iota(jnp.int32, (seq, seq), 1)
    causal = jnp.concatenate([qi >= ki] * groups, axis=0)

    @pl.loop(0, kv_heads)
    def _(kvh):
        for b in range(n_seq):
            rs = pl.ds(b * seq, seq)
            kk = qkv[rs, pl.ds(pl.multiple_of(qdim + kvh * 128, 128), 128)]
            vv = qkv[rs, pl.ds(pl.multiple_of(qdim + (kv_heads + kvh) * 128, 128), 128)]
            qcols = [pl.ds(pl.multiple_of((kvh * groups + i) * 128, 128), 128) for i in range(groups)]
            qq = jnp.concatenate([qkv[rs, c] for c in qcols], axis=0)
            s = lax.dot_general(qq, kk, (((1,), (1,)), ((), ())), preferred_element_type=F32) * 128 ** -0.5
            s = jnp.where(causal, s, -jnp.inf)
            e = jnp.exp(s - jnp.max(s, axis=-1, keepdims=True))
            p = (e * (1.0 / jnp.sum(e, axis=-1, keepdims=True))).astype(BF16)
            o = jnp.dot(p, vv, preferred_element_type=F32).astype(BF16)
            for i, c in enumerate(qcols):
                qkv[rs, c] = o[i * seq:(i + 1) * seq]

    def wo_body(t, w0, w1):
        acc = jnp.dot(qkv[:, :half_q], w0[...], preferred_element_type=F32)
        acc += jnp.dot(qkv[:, half_q:qdim], w1[...], preferred_element_type=F32)
        h[:, cols(t)] = (h[:, cols(t)].astype(F32) + acc).astype(BF16)

    phase(u_wo, dim // WN, wo_body, 2)
    norm_rows(mlp_g)

    def gu_body(t, w0, w1):
        g = jnp.dot(a[...], w0[...], preferred_element_type=F32)
        u = jnp.dot(a[...], w1[...], preferred_element_type=F32)
        act[:, cols(t)] = (silu(g) * u).astype(BF16)

    phase(u_gu, ff // WN, gu_body, 2)

    def dn_body(t, *ws):
        acc = None
        for (s, n), w in zip(chunks(ff), ws):
            d = jnp.dot(act[:, s:s + n], w[...], preferred_element_type=F32)
            acc = d if acc is None else acc + d
        h[:, cols(t)] = (h[:, cols(t)].astype(F32) + acc).astype(BF16)

    phase(u_dn, dim // WN, dn_body)
    norm_rows(mamba_g)

    row_id = lax.broadcasted_iota(jnp.int32, (seq, 1), 0)

    def scatter(dst, r0, t, val):
        for j in range(WN // 128):
            for i in range(seq // 8):
                dst[pl.ds((r0 + i * 8) * PITCH + t * (WN // 128) + j, 8, stride=PITCH), :] = (
                    val[i * 8:(i + 1) * 8, j * 128:(j + 1) * 128])

    def wx_body(t, w):
        res = jnp.dot(a[...], w[...], preferred_element_type=F32).astype(BF16).astype(F32)
        for b in range(n_seq):
            xi = res[b * seq:(b + 1) * seq]
            acc = chan[4:5, cols(t)] + chan[CONV - 1:CONV, cols(t)] * xi
            for j in range(CONV - 1):
                back = CONV - 1 - j
                prev = jnp.where(row_id >= back, pltpu.roll(xi, back, axis=0), 0.0)
                acc += chan[j:j + 1, cols(t)] * prev
            c = silu(acc).astype(BF16)
            act[b * seq:(b + 1) * seq, cols(t)] = c
            scatter(xs, b * seq, t, c.astype(F32))

    phase(u_wx, inner // WN, wx_body)

    in_copies[0].wait()
    r = lax.dot_general(act[:, :inner], wxp[...], (((1,), (1,)), ((), ())), preferred_element_type=F32)
    n_r = r.shape[1]
    gain_r = jnp.concatenate([dt_g[...].reshape(1, dt_rank), b_g[...].reshape(1, n_state), c_g[...].reshape(1, n_state)], axis=1)
    col = lax.broadcasted_iota(jnp.int32, (1, n_r), 1)
    sq = r * r

    def inv_of(mask, n):
        return lax.rsqrt(jnp.sum(jnp.where(mask, sq, 0.0), axis=-1, keepdims=True) * (1.0 / n) + EPS)

    m_dt = col < dt_rank
    m_b = (col >= dt_rank) & (col < dt_rank + n_state)
    m_c = col >= dt_rank + n_state
    inv = jnp.where(m_dt, inv_of(m_dt, dt_rank), jnp.where(m_b, inv_of(m_b, n_state), inv_of(m_c, n_state)))
    rn = r * inv * gain_r
    rn_ref[...] = rn
    dt_in = rn[:, :dt_rank].astype(BF16)
    act[:, inner:inner + dt_rank] = dt_in
    in_copies[1].wait()

    @pl.loop(0, inner // WN)
    def _(t):
        pre = jnp.dot(act[:, inner:inner + dt_rank], wdt[:, cols(t)], preferred_element_type=F32) + chan[5:6, cols(t)]
        step = jnp.maximum(pre, 0.0) + jnp.log1p(jnp.exp(-jnp.abs(pre)))
        for b in range(n_seq):
            scatter(delta, b * seq, t, step[b * seq:(b + 1) * seq])

    def bcast(ref, idx):
        return jnp.broadcast_to(ref[pl.ds(idx, 1), :], (8, 128))

    toks = 8
    kc = 512
    n_zk = dim // kc
    n_ok = inner // kc
    n_chunk = lanes // 8
    z_per = inner // WN // n_chunk

    def send_out(b, t):
        a[b * seq:(b + 1) * seq, cols(t)] = (
            h[b * seq:(b + 1) * seq, cols(t)].astype(F32) + acc_ref[b * seq:(b + 1) * seq, :]).astype(BF16)
        exchange(lambda p, b: a.at[blk(p, b), cols(t)], lambda p, b: out_ref.at[p * n_seq + b, :, cols(t)], 1, [b])

    for b in range(n_seq):
        for n in range(n_state):
            for ref, c0 in ((bb, dt_rank + n), (cb, dt_rank + n_state + n)):
                ref[n * seq:(n + 1) * seq, :] = jnp.broadcast_to(rn_ref[b * seq:(b + 1) * seq, c0:c0 + 1], (seq, 128))

        @pl.loop(0, n_chunk)
        def _(c, b=b):
            av = [a2[pl.ds(n * PITCH + c * 8, 8), :] for n in range(n_state)]
            dsk = dskip[pl.ds(pl.multiple_of(c * 8, 8), 8), :]

            def tokens(i, st):
                st = list(st)
                for k in range(toks):
                    r = i * toks + k
                    at = pl.ds((b * seq + r) * PITCH + c * 8, 8)
                    d = delta[at, :]
                    x = xs[at, :]
                    dx = d * x
                    terms = []
                    for n in range(n_state):
                        st[n] = jnp.exp2(d * av[n]) * st[n] + dx * bcast(bb, n * seq + r)
                        terms.append(st[n] * bcast(cb, n * seq + r))
                    terms.append(dsk * x)
                    while len(terms) > 1:
                        terms = [terms[m] + terms[m + 1] for m in range(0, len(terms) - 1, 2)] + (
                            [terms[-1]] if len(terms) % 2 else [])
                    delta[at, :] = terms[0]
                return tuple(st)

            st = tuple(jnp.zeros((8, 128), F32) for _ in range(n_state))
            if b == 0:
                for j in range(z_per):
                    u = u_wz + c * z_per + j
                    slot = lax.rem(u, SLOTS)
                    copy((wz, 0, dim), 0, slot).wait()
                    acc_ref[...] = jnp.zeros_like(acc_ref)

                    def piece(k, st, slot=slot, j=j):
                        ks = pl.ds(pl.multiple_of(k * kc, kc), kc)
                        acc_ref[...] += jnp.dot(a[:, ks], ring[slot, ks, :], preferred_element_type=F32)
                        return tokens(j * n_zk + k, st)

                    st = lax.fori_loop(0, n_zk, piece, st)
                    qkv[:, cols(c * z_per + j)] = acc_ref[...].astype(BF16)
                    start(u + SLOTS, u_wz + SLOTS, u_out + SLOTS)
                done = z_per * n_zk
            else:
                for j in range(2):
                    copy((wout, 0, unit), 0, lax.rem(u_out + c * 2 + j, SLOTS)).wait()
                acc_ref[:seq, :] = jnp.zeros((seq, WN), F32)

                def piece(k, st):
                    half = n_ok // 2
                    slot = lax.rem(u_out + c * 2 + lax.div(k, half), SLOTS)
                    ks = pl.ds(pl.multiple_of(k * kc, kc), kc)
                    kw = pl.ds(pl.multiple_of(lax.rem(k, half) * kc, kc), kc)
                    acc_ref[:seq, :] += jnp.dot(act[:seq, ks], ring[slot, kw, :], preferred_element_type=F32)
                    return tokens(k, st)

                st = lax.fori_loop(0, n_ok, piece, st)
                send_out(0, c)
                done = n_ok
            lax.fori_loop(done, seq // toks, tokens, st)

        @pl.loop(0, seq // 16)
        def _(i, b=b):
            r0 = pl.multiple_of(b * seq + i * 16, 16)
            for j in range(lanes):
                y = jnp.concatenate([delta[pl.ds((r0 + 8 * m) * PITCH + j, 8, stride=PITCH), :] for m in range(2)], axis=0)
                z = qkv[pl.ds(r0, 16), j * 128:(j + 1) * 128].astype(F32)
                act[pl.ds(r0, 16), j * 128:(j + 1) * 128] = (y * silu(z)).astype(BF16)

    for t in range(dim // WN):
        acc = None
        for j, (s, n) in enumerate(chunks(inner)):
            d = jnp.dot(act[seq:, s:s + n], ring[(u_out + 2 * t + j) % SLOTS, :n], preferred_element_type=F32)
            acc = d if acc is None else acc + d
        acc_ref[seq:, :] = acc
        send_out(1, t)
    exchange_wait(out_ref, a.at[pl.ds(0, rows - n_seq * tok)], 1)


def layer_pair(hidden, attn_norm, w_q, w_k, w_v, w_o, mlp_norm, w_gate, w_up, w_down, mamba_norm, w_in_x, w_in_z, conv_w, conv_b, w_xproj, dt_norm, b_norm, c_norm, w_dt, dt_bias, a_log, d_skip, w_out):
    n_batch, tok, dim = hidden.shape
    n_seq = n_batch // lax.axis_size("sp")
    rows = n_batch * tok
    inner, n_state = a_log.shape
    hbm = pl.BlockSpec(memory_space=pltpu.HBM)
    vm = pl.BlockSpec(memory_space=pltpu.VMEM)
    qkv_dim = (w_q.shape[1] + w_k.shape[1] + w_v.shape[1]) * 128
    return pl.pallas_call(
        block_kernel,
        out_shape=jax.ShapeDtypeStruct(hidden.shape, BF16),
        in_specs=[hbm] * 13 + [vm] * 11,
        out_specs=hbm,
        scratch_shapes=[
            pltpu.VMEM((SLOTS, dim, WN), BF16),
            pltpu.VMEM((STAGE, KB, 32, 128), BF16),
            pltpu.VMEM((rows, WN), F32),
            pltpu.VMEM((rows, qkv_dim), BF16),
            pltpu.VMEM((rows, dim), BF16),
            pltpu.VMEM((rows, dim), BF16),
            pltpu.VMEM((rows, w_gate.shape[1]), BF16),
            pltpu.VMEM((rows * PITCH, 128), F32),
            pltpu.VMEM((rows * PITCH, 128), F32),
            pltpu.VMEM((128 * n_state, 128), F32),
            pltpu.VMEM((128 * n_state, 128), F32),
            pltpu.VMEM((w_xproj.shape[1], inner), BF16),
            pltpu.VMEM(w_dt.shape, BF16),
            pltpu.VMEM((n_state * PITCH, 128), F32),
            pltpu.VMEM((8, inner), F32),
            pltpu.VMEM((rows, w_xproj.shape[1]), F32),
            pltpu.SemaphoreType.DMA((SLOTS,)),
            pltpu.SemaphoreType.DMA((STAGE,)),
            pltpu.SemaphoreType.DMA((2,)),
            pltpu.SemaphoreType.DMA((2,)),
            pltpu.SemaphoreType.DMA((2,)),
        ],
        compiler_params=pltpu.CompilerParams(vmem_limit_bytes=67043328, collective_id=0, has_side_effects=True),
        name="block",
    )(hidden, w_q.reshape(-1, 32, 128), w_k.reshape(-1, 32, 128), w_v.reshape(-1, 32, 128), w_o.reshape(-1, dim),
      w_gate, w_up, w_down, w_in_x, w_in_z, w_xproj.T, w_dt, w_out, attn_norm, mlp_norm, mamba_norm, conv_w, conv_b,
      dt_norm, b_norm, c_norm, dt_bias, d_skip.reshape(-1, 128), a_log.T)


def solution(mesh):
    act_spec = P("dp", "sp", None)
    return jax.shard_map(
        layer_pair,
        mesh=mesh,
        in_specs=(act_spec,) + (P(),) * 23,
        out_specs=act_spec,
        check_vma=False,
    )
```

```python
import functools
import math
import jax
import jax.numpy as jnp
from jax import lax
from jax.experimental import pallas as pl
from jax.experimental.pallas import tpu as pltpu
from jax.sharding import PartitionSpec as P

EPS = 1e-6
CONV = 4
SLOTS = 12
STAGE = 6
KB = 64
WN = 512
PITCH = 41
F32 = jnp.float32
BF16 = jnp.bfloat16
LOG2E = math.log2(math.e)


def rms_scale(values, gain_vec):
    values_f = values.astype(F32)
    inv_rms = lax.rsqrt(jnp.mean(values_f * values_f, axis=-1, keepdims=True) + EPS)
    return values_f * inv_rms * gain_vec.astype(F32)


def silu(v):
    half = 0.5 * v
    return half + half * jnp.tanh(half)


def block_kernel(x_hbm, wq, wk, wv, wo, wg, wu, wd, wx, wz, wxp_hbm, wdt_hbm, wout,
                 attn_g, mlp_g, mamba_g, conv_w, conv_b, dt_g, b_g, c_g, dt_b, dskip, a_log, out_ref,
                 ring, stage, qkv, h, a, act, delta, xs, bb, cb, wxp, wdt, a2, chan, rn_ref,
                 ring_sem, stage_sem, in_sem, send_sem, recv_sem):
    rows, dim = h.shape
    n_seq, seq = 2, 128
    n_dev = x_hbm.shape[0] // n_seq
    tok = x_hbm.shape[1]
    me = lax.axis_index("sp")
    inner = wx.shape[1]
    ff = wg.shape[1]
    qdim = wo.shape[0]
    heads = qdim // 128
    kv_heads = (qkv.shape[1] - qdim) // 256
    groups = heads // kv_heads
    lanes = inner // 128
    n_state = a_log.shape[0]
    dt_rank = wdt.shape[0]
    unit = ring.shape[1]

    def chunks(total):
        return [(s, min(unit, total - s)) for s in range(0, total, unit)]

    def cols(t):
        return pl.ds(pl.multiple_of(t * WN, WN), WN)

    segs = []
    base = 0

    def add_seg(n_tiles, parts):
        nonlocal base
        first = base
        base = first + n_tiles * len(parts)
        segs.append((first, base, parts))
        return first

    half_q = qdim // 2
    u_qkv = add_seg(qkv.shape[1] // WN, [(None, 0, dim)])
    u_wo = add_seg(dim // WN, [(wo, 0, half_q), (wo, half_q, half_q)])
    u_gu = add_seg(ff // WN, [(wg, 0, dim), (wu, 0, dim)])
    u_dn = add_seg(dim // WN, [(wd, s, n) for s, n in chunks(ff)])
    u_wx = add_seg(inner // WN, [(wx, 0, dim)])
    u_wz = add_seg(inner // WN, [(wz, 0, dim)])
    u_out = add_seg(dim // WN, [(wout, s, n) for s, n in chunks(inner)])

    def copy(part, tile, slot):
        w, r0, nr = part
        return pltpu.make_async_copy(w.at[pl.ds(r0, nr), cols(tile)], ring.at[slot, pl.ds(0, nr)], ring_sem.at[slot])

    def start(u, lo, hi):
        for first, last, parts in segs:
            if hi < first or lo >= last or parts[0][0] is None:
                continue
            n = len(parts)
            for i, part in enumerate(parts):
                @pl.when((u >= first) & (u < last) & (lax.rem(u - first + n, n) == i))
                def _(part=part, first=first, n=n):
                    copy(part, lax.div(u - first, n), lax.rem(u, SLOTS)).start()

    def phase(first, n_tiles, body, per=1):
        parts = [s for s in segs if s[0] == first][0][2]
        n = len(parts)

        def group(t0, count):
            views = []
            for u in range(count * n):
                slot = lax.rem(first + t0 * n + u, SLOTS)
                part = parts[u % n]
                if part[0] is not None:
                    copy(part, 0, slot).wait()
                views.append(ring.at[slot, pl.ds(0, part[2])])
            for m in range(count):
                body(t0 + m, *views[m * n:(m + 1) * n])
            for u in range(count * n):
                start(first + t0 * n + u + SLOTS, first + SLOTS, first + SLOTS + n_tiles * n - 1)

        @pl.loop(0, n_tiles // per)
        def _(g):
            group(g * per, per)

        if n_tiles % per:
            group(jnp.int32(n_tiles - n_tiles % per), n_tiles % per)

    def norm_rows(g_ref):
        gain = g_ref[...].astype(F32).reshape(1, dim)

        @pl.loop(0, rows // 32)
        def _(i):
            rs = pl.ds(pl.multiple_of(i * 32, 32), 32)
            hv = h[rs, :].astype(F32)
            inv = lax.rsqrt(jnp.mean(hv * hv, axis=-1, keepdims=True) + EPS)
            a[rs, :] = (hv * inv * gain).astype(BF16)

    in_copies = [
        pltpu.make_async_copy(wxp_hbm, wxp, in_sem.at[0]),
        pltpu.make_async_copy(wdt_hbm, wdt, in_sem.at[1]),
    ]
    n_q = wq.shape[0] // KB
    n_kv = wk.shape[0] // KB

    def stage_copy(w, c, slot):
        return pltpu.make_async_copy(w.at[pl.ds(c * KB, KB)], stage.at[slot], stage_sem.at[slot])

    def stage_start(i):
        slot = lax.rem(i, STAGE)
        for w, lo, n in ((wq, 0, n_q), (wk, n_q, n_kv), (wv, n_q + n_kv, n_kv)):
            @pl.when((i >= lo) & (i < lo + n))
            def _(w=w, lo=lo):
                stage_copy(w, i - lo, slot).start()

    for i in range(STAGE):
        stage_start(jnp.int32(i))

    barrier = pltpu.get_barrier_semaphore()
    for d in range(1, n_dev):
        pl.semaphore_signal(barrier, inc=1, device_id={"sp": lax.rem(me + d, n_dev)}, device_id_type=pl.DeviceIdType.MESH)
    pl.semaphore_wait(barrier, n_dev - 1)

    def exchange(src_of, dst_of, ex, bs):
        for d in range(1, n_dev):
            peer = lax.rem(me + d, n_dev)
            for b in bs:
                pltpu.make_async_remote_copy(
                    src_ref=src_of(peer, b), dst_ref=dst_of(me, b), send_sem=send_sem.at[ex], recv_sem=recv_sem.at[ex],
                    device_id={"sp": peer}, device_id_type=pl.DeviceIdType.MESH).start()
        for b in bs:
            pltpu.make_async_copy(src_of(me, b), dst_of(me, b), recv_sem.at[ex]).start()

    def exchange_wait(whole_dst, part_src, ex):
        pltpu.make_async_copy(whole_dst, whole_dst, recv_sem.at[ex]).wait()
        pltpu.make_async_copy(part_src, part_src, send_sem.at[ex]).wait()

    def blk(owner, b):
        return pl.ds(pl.multiple_of(b * seq + owner * tok, tok), tok)

    exchange(lambda p, b: x_hbm.at[p * n_seq + b], lambda p, b: h.at[blk(p, b)], 0, range(n_seq))
    for c in in_copies:
        c.start()

    chan[0:CONV, :] = conv_w[...].astype(F32)
    chan[CONV:CONV + 1, :] = conv_b[...].astype(F32).reshape(1, inner)
    chan[CONV + 1:CONV + 2, :] = dt_b[...].reshape(1, inner)
    for j in range(lanes):
        neg = -jnp.exp(a_log[:, j * 128:(j + 1) * 128]) * LOG2E
        for m in range(n_state // 8):
            a2[pl.ds(m * 8 * PITCH + j, 8, stride=PITCH), :] = neg[m * 8:(m + 1) * 8]

    def relayout(i, n_heads, unit0, k0):
        slot = lax.rem(i, STAGE)
        per = 32 // n_heads
        pitch = n_heads + 1
        stage_copy(wq, 0, slot).wait()

        @pl.loop(0, KB * per // 32)
        def _(g2):
            for m in range(2):
                g = g2 * 2 + m
                base_row = m * 16 * 33
                for r in range(16 // per):
                    val = stage[slot, g * (16 // per) + r].astype(F32)
                    for j in range(per):
                        delta[pl.ds(base_row + (r * per + j) * pitch, n_heads), :] = val[j * n_heads:(j + 1) * n_heads]
                ks = pl.ds(pl.multiple_of(k0 + g * 16, 16), 16)
                for hd in range(n_heads):
                    w = WN // 128
                    ring[unit0 + hd // w, ks, (hd % w) * 128:(hd % w + 1) * 128] = (
                        delta[pl.ds(base_row + hd, 16, stride=pitch), :].astype(BF16))

        stage_start(i + STAGE)

    @pl.loop(0, n_q)
    def _(i):
        relayout(i, heads, 0, i * KB)

    for m in range(2):
        @pl.loop(0, n_kv)
        def _(i, m=m):
            relayout(n_q + m * n_kv + i, kv_heads, (qdim + m * kv_heads * 128) // WN, i * KB * (32 // kv_heads))

    exchange_wait(h, h.at[pl.ds(0, rows - n_seq * tok)], 0)
    norm_rows(attn_g)

    def qkv_body(t, w):
        qkv[:, cols(t)] = jnp.dot(a[...], w[...], preferred_element_type=F32).astype(BF16)

    phase(u_qkv, qkv.shape[1] // WN, qkv_body, 3)

    qi = lax.broadcasted_iota(jnp.int32, (seq, seq), 0)
    ki = lax.broadcasted_iota(jnp.int32, (seq, seq), 1)
    causal = jnp.concatenate([qi >= ki] * groups, axis=0)

    @pl.loop(0, kv_heads)
    def _(kvh):
        for b in range(n_seq):
            rs = pl.ds(b * seq, seq)
            kk = qkv[rs, pl.ds(pl.multiple_of(qdim + kvh * 128, 128), 128)]
            vv = qkv[rs, pl.ds(pl.multiple_of(qdim + (kv_heads + kvh) * 128, 128), 128)]
            qcols = [pl.ds(pl.multiple_of((kvh * groups + i) * 128, 128), 128) for i in range(groups)]
            qq = jnp.concatenate([qkv[rs, c] for c in qcols], axis=0)
            s = lax.dot_general(qq, kk, (((1,), (1,)), ((), ())), preferred_element_type=F32) * 128 ** -0.5
            s = jnp.where(causal, s, -jnp.inf)
            e = jnp.exp(s - jnp.max(s, axis=-1, keepdims=True))
            p = (e * (1.0 / jnp.sum(e, axis=-1, keepdims=True))).astype(BF16)
            o = jnp.dot(p, vv, preferred_element_type=F32).astype(BF16)
            for i, c in enumerate(qcols):
                qkv[rs, c] = o[i * seq:(i + 1) * seq]

    def wo_body(t, w0, w1):
        acc = jnp.dot(qkv[:, :half_q], w0[...], preferred_element_type=F32)
        acc += jnp.dot(qkv[:, half_q:qdim], w1[...], preferred_element_type=F32)
        h[:, cols(t)] = (h[:, cols(t)].astype(F32) + acc).astype(BF16)

    phase(u_wo, dim // WN, wo_body, 2)
    norm_rows(mlp_g)

    def gu_body(t, w0, w1):
        g = jnp.dot(a[...], w0[...], preferred_element_type=F32)
        u = jnp.dot(a[...], w1[...], preferred_element_type=F32)
        act[:, cols(t)] = (silu(g) * u).astype(BF16)

    phase(u_gu, ff // WN, gu_body, 2)

    def dn_body(t, *ws):
        acc = None
        for (s, n), w in zip(chunks(ff), ws):
            d = jnp.dot(act[:, s:s + n], w[...], preferred_element_type=F32)
            acc = d if acc is None else acc + d
        h[:, cols(t)] = (h[:, cols(t)].astype(F32) + acc).astype(BF16)

    phase(u_dn, dim // WN, dn_body)
    norm_rows(mamba_g)

    row_id = lax.broadcasted_iota(jnp.int32, (seq, 1), 0)

    def scatter(dst, r0, t, val):
        for j in range(WN // 128):
            for i in range(seq // 8):
                dst[pl.ds((r0 + i * 8) * PITCH + t * (WN // 128) + j, 8, stride=PITCH), :] = (
                    val[i * 8:(i + 1) * 8, j * 128:(j + 1) * 128])

    def wx_body(t, w):
        res = jnp.dot(a[...], w[...], preferred_element_type=F32).astype(BF16).astype(F32)
        for b in range(n_seq):
            xi = res[b * seq:(b + 1) * seq]
            acc = chan[4:5, cols(t)] + chan[CONV - 1:CONV, cols(t)] * xi
            for j in range(CONV - 1):
                back = CONV - 1 - j
                prev = jnp.where(row_id >= back, pltpu.roll(xi, back, axis=0), 0.0)
                acc += chan[j:j + 1, cols(t)] * prev
            c = silu(acc).astype(BF16)
            act[b * seq:(b + 1) * seq, cols(t)] = c
            scatter(xs, b * seq, t, c.astype(F32))

    phase(u_wx, inner // WN, wx_body, 2)

    in_copies[0].wait()
    r = lax.dot_general(act[:, :inner], wxp[...], (((1,), (1,)), ((), ())), preferred_element_type=F32)
    n_r = r.shape[1]
    gain_r = jnp.concatenate([dt_g[...].reshape(1, dt_rank), b_g[...].reshape(1, n_state), c_g[...].reshape(1, n_state)], axis=1)
    col = lax.broadcasted_iota(jnp.int32, (1, n_r), 1)
    sq = r * r

    def inv_of(mask, n):
        return lax.rsqrt(jnp.sum(jnp.where(mask, sq, 0.0), axis=-1, keepdims=True) * (1.0 / n) + EPS)

    m_dt = col < dt_rank
    m_b = (col >= dt_rank) & (col < dt_rank + n_state)
    m_c = col >= dt_rank + n_state
    inv = jnp.where(m_dt, inv_of(m_dt, dt_rank), jnp.where(m_b, inv_of(m_b, n_state), inv_of(m_c, n_state)))
    rn = r * inv * gain_r
    rn_ref[...] = rn
    dt_in = rn[:, :dt_rank].astype(BF16)
    act[:, inner:inner + dt_rank] = dt_in
    in_copies[1].wait()

    def wz_body(t, w):
        pre = jnp.dot(act[:, inner:inner + dt_rank], wdt[:, cols(t)], preferred_element_type=F32)
        qkv[:, cols(t)] = jnp.dot(a[...], w[...], preferred_element_type=F32).astype(BF16)
        pre = pre + chan[5:6, cols(t)]
        step = jnp.maximum(pre, 0.0) + jnp.log1p(jnp.exp(-jnp.abs(pre)))
        for b in range(n_seq):
            scatter(delta, b * seq, t, step[b * seq:(b + 1) * seq])

    phase(u_wz, inner // WN, wz_body, 2)

    def bcast(ref, idx):
        return jnp.broadcast_to(ref[pl.ds(idx, 1), :], (8, 128))

    toks = 8

    for b in range(n_seq):
        for n in range(n_state):
            for ref, c0 in ((bb, dt_rank + n), (cb, dt_rank + n_state + n)):
                ref[n * seq:(n + 1) * seq, :] = jnp.broadcast_to(rn_ref[b * seq:(b + 1) * seq, c0:c0 + 1], (seq, 128))

        @pl.loop(0, lanes // 8)
        def _(c, b=b):
            av = [a2[pl.ds(n * PITCH + c * 8, 8), :] for n in range(n_state)]
            dsk = dskip[pl.ds(pl.multiple_of(c * 8, 8), 8), :]

            def tokens(i, st):
                st = list(st)
                for k in range(toks):
                    r = i * toks + k
                    at = pl.ds((b * seq + r) * PITCH + c * 8, 8)
                    d = delta[at, :]
                    x = xs[at, :]
                    dx = d * x
                    terms = []
                    for n in range(n_state):
                        st[n] = jnp.exp2(d * av[n]) * st[n] + dx * bcast(bb, n * seq + r)
                        terms.append(st[n] * bcast(cb, n * seq + r))
                    terms.append(dsk * x)
                    while len(terms) > 1:
                        terms = [terms[m] + terms[m + 1] for m in range(0, len(terms) - 1, 2)] + (
                            [terms[-1]] if len(terms) % 2 else [])
                    delta[at, :] = terms[0]
                return tuple(st)

            st = tuple(jnp.zeros((8, 128), F32) for _ in range(n_state))
            lax.fori_loop(0, seq // toks, tokens, st)

        @pl.loop(0, seq // 16)
        def _(i, b=b):
            r0 = pl.multiple_of(b * seq + i * 16, 16)
            for j in range(lanes):
                y = jnp.concatenate([delta[pl.ds((r0 + 8 * m) * PITCH + j, 8, stride=PITCH), :] for m in range(2)], axis=0)
                z = qkv[pl.ds(r0, 16), j * 128:(j + 1) * 128].astype(F32)
                act[pl.ds(r0, 16), j * 128:(j + 1) * 128] = (y * silu(z)).astype(BF16)

        rs = pl.ds(b * seq, seq)
        @pl.loop(0, dim // WN)
        def _(t, b=b, rs=rs):
            views = []
            for j, (s, n) in enumerate(chunks(inner)):
                slot = lax.rem(u_out + 2 * t + j, SLOTS)
                if b == 0:
                    copy((wout, s, n), 0, slot).wait()
                views.append(jnp.dot(act[rs, s:s + n], ring[slot, :n], preferred_element_type=F32))
            a[rs, cols(t)] = (h[rs, cols(t)].astype(F32) + (views[0] + views[1])).astype(BF16)
            exchange(lambda p, b: a.at[blk(p, b), cols(t)], lambda p, b: out_ref.at[p * n_seq + b, :, cols(t)], 1, [b])

    exchange_wait(out_ref, a.at[pl.ds(0, rows - n_seq * tok)], 1)


def layer_pair(hidden, attn_norm, w_q, w_k, w_v, w_o, mlp_norm, w_gate, w_up, w_down, mamba_norm, w_in_x, w_in_z, conv_w, conv_b, w_xproj, dt_norm, b_norm, c_norm, w_dt, dt_bias, a_log, d_skip, w_out):
    n_batch, tok, dim = hidden.shape
    n_seq = n_batch // lax.axis_size("sp")
    rows = n_batch * tok
    inner, n_state = a_log.shape
    hbm = pl.BlockSpec(memory_space=pltpu.HBM)
    vm = pl.BlockSpec(memory_space=pltpu.VMEM)
    qkv_dim = (w_q.shape[1] + w_k.shape[1] + w_v.shape[1]) * 128
    return pl.pallas_call(
        block_kernel,
        out_shape=jax.ShapeDtypeStruct(hidden.shape, BF16),
        in_specs=[hbm] * 13 + [vm] * 11,
        out_specs=hbm,
        scratch_shapes=[
            pltpu.VMEM((SLOTS, dim, WN), BF16),
            pltpu.VMEM((STAGE, KB, 32, 128), BF16),
            pltpu.VMEM((rows, qkv_dim), BF16),
            pltpu.VMEM((rows, dim), BF16),
            pltpu.VMEM((rows, dim), BF16),
            pltpu.VMEM((rows, w_gate.shape[1]), BF16),
            pltpu.VMEM((rows * PITCH, 128), F32),
            pltpu.VMEM((rows * PITCH, 128), F32),
            pltpu.VMEM((128 * n_state, 128), F32),
            pltpu.VMEM((128 * n_state, 128), F32),
            pltpu.VMEM((w_xproj.shape[1], inner), BF16),
            pltpu.VMEM(w_dt.shape, BF16),
            pltpu.VMEM((n_state * PITCH, 128), F32),
            pltpu.VMEM((8, inner), F32),
            pltpu.VMEM((rows, w_xproj.shape[1]), F32),
            pltpu.SemaphoreType.DMA((SLOTS,)),
            pltpu.SemaphoreType.DMA((STAGE,)),
            pltpu.SemaphoreType.DMA((2,)),
            pltpu.SemaphoreType.DMA((2,)),
            pltpu.SemaphoreType.DMA((2,)),
        ],
        compiler_params=pltpu.CompilerParams(vmem_limit_bytes=67043328, collective_id=0, has_side_effects=True),
        name="block",
    )(hidden, w_q.reshape(-1, 32, 128), w_k.reshape(-1, 32, 128), w_v.reshape(-1, 32, 128), w_o.reshape(-1, dim),
      w_gate, w_up, w_down, w_in_x, w_in_z, w_xproj.T, w_dt, w_out, attn_norm, mlp_norm, mamba_norm, conv_w, conv_b,
      dt_norm, b_norm, c_norm, dt_bias, d_skip.reshape(-1, 128), a_log.T)


def solution(mesh):
    act_spec = P("dp", "sp", None)
    return jax.shard_map(
        layer_pair,
        mesh=mesh,
        in_specs=(act_spec,) + (P(),) * 23,
        out_specs=act_spec,
        check_vma=False,
    )
```

```python
import functools
import math
import jax
import jax.numpy as jnp
from jax import lax
from jax.experimental import pallas as pl
from jax.experimental.pallas import tpu as pltpu
from jax.sharding import PartitionSpec as P

EPS = 1e-6
CONV = 4
SLOTS = 12
STAGE = 6
KB = 64
WN = 512
PITCH = 41
F32 = jnp.float32
BF16 = jnp.bfloat16
LOG2E = math.log2(math.e)


def rms_scale(values, gain_vec):
    values_f = values.astype(F32)
    inv_rms = lax.rsqrt(jnp.mean(values_f * values_f, axis=-1, keepdims=True) + EPS)
    return values_f * inv_rms * gain_vec.astype(F32)


def silu(v):
    half = 0.5 * v
    return half + half * jnp.tanh(half)


def block_kernel(x_hbm, wq, wk, wv, wo, wg, wu, wd, wx, wz, wxp_hbm, wdt_hbm, wout,
                 attn_g, mlp_g, mamba_g, conv_w, conv_b, dt_g, b_g, c_g, dt_b, dskip, a_log, out_ref,
                 ring, stage, qkv, h, a, act, delta, xs, bb, cb, wxp, wdt, a2, chan, rn_ref,
                 ring_sem, stage_sem, in_sem, send_sem, recv_sem):
    rows, dim = h.shape
    n_seq, seq = 2, 128
    n_dev = x_hbm.shape[0] // n_seq
    tok = x_hbm.shape[1]
    me = lax.axis_index("sp")
    inner = wx.shape[1]
    ff = wg.shape[1]
    qdim = wo.shape[0]
    heads = qdim // 128
    kv_heads = (qkv.shape[1] - qdim) // 256
    groups = heads // kv_heads
    lanes = inner // 128
    n_state = a_log.shape[0]
    dt_rank = wdt.shape[0]
    unit = ring.shape[1]

    def chunks(total):
        return [(s, min(unit, total - s)) for s in range(0, total, unit)]

    def cols(t):
        return pl.ds(pl.multiple_of(t * WN, WN), WN)

    segs = []
    base = 0

    def add_seg(n_tiles, parts):
        nonlocal base
        first = base
        base = first + n_tiles * len(parts)
        segs.append((first, base, parts))
        return first

    half_q = qdim // 2
    u_qkv = add_seg(qkv.shape[1] // WN, [(None, 0, dim)])
    u_wo = add_seg(dim // WN, [(wo, 0, half_q), (wo, half_q, half_q)])
    u_gu = add_seg(ff // WN, [(wg, 0, dim), (wu, 0, dim)])
    u_dn = add_seg(dim // WN, [(wd, s, n) for s, n in chunks(ff)])
    u_wx = add_seg(inner // WN, [(wx, 0, dim)])
    u_wz = add_seg(inner // WN, [(wz, 0, dim)])
    u_out = add_seg(dim // WN, [(wout, s, n) for s, n in chunks(inner)])

    def copy(part, tile, slot):
        w, r0, nr = part
        return pltpu.make_async_copy(w.at[pl.ds(r0, nr), cols(tile)], ring.at[slot, pl.ds(0, nr)], ring_sem.at[slot])

    def start(u, lo, hi):
        for first, last, parts in segs:
            if hi < first or lo >= last or parts[0][0] is None:
                continue
            n = len(parts)
            for i, part in enumerate(parts):
                @pl.when((u >= first) & (u < last) & (lax.rem(u - first + n, n) == i))
                def _(part=part, first=first, n=n):
                    copy(part, lax.div(u - first, n), lax.rem(u, SLOTS)).start()

    def phase(first, n_tiles, body, per=1):
        parts = [s for s in segs if s[0] == first][0][2]
        n = len(parts)

        def group(t0, count):
            views = []
            for u in range(count * n):
                slot = lax.rem(first + t0 * n + u, SLOTS)
                part = parts[u % n]
                if part[0] is not None:
                    copy(part, 0, slot).wait()
                views.append(ring.at[slot, pl.ds(0, part[2])])
            for m in range(count):
                body(t0 + m, *views[m * n:(m + 1) * n])
            for u in range(count * n):
                start(first + t0 * n + u + SLOTS, first + SLOTS, first + SLOTS + n_tiles * n - 1)

        @pl.loop(0, n_tiles // per)
        def _(g):
            group(g * per, per)

        if n_tiles % per:
            group(jnp.int32(n_tiles - n_tiles % per), n_tiles % per)

    def norm_rows(g_ref):
        gain = g_ref[...].astype(F32).reshape(1, dim)

        @pl.loop(0, rows // 32)
        def _(i):
            rs = pl.ds(pl.multiple_of(i * 32, 32), 32)
            hv = h[rs, :].astype(F32)
            inv = lax.rsqrt(jnp.mean(hv * hv, axis=-1, keepdims=True) + EPS)
            a[rs, :] = (hv * inv * gain).astype(BF16)

    in_copies = [
        pltpu.make_async_copy(wxp_hbm, wxp, in_sem.at[0]),
        pltpu.make_async_copy(wdt_hbm, wdt, in_sem.at[1]),
    ]
    n_q = wq.shape[0] // KB
    n_kv = wk.shape[0] // KB

    def stage_copy(w, c, slot):
        return pltpu.make_async_copy(w.at[pl.ds(c * KB, KB)], stage.at[slot], stage_sem.at[slot])

    def stage_start(i):
        slot = lax.rem(i, STAGE)
        for w, lo, n in ((wq, 0, n_q), (wk, n_q, n_kv), (wv, n_q + n_kv, n_kv)):
            @pl.when((i >= lo) & (i < lo + n))
            def _(w=w, lo=lo):
                stage_copy(w, i - lo, slot).start()

    for i in range(STAGE):
        stage_start(jnp.int32(i))

    barrier = pltpu.get_barrier_semaphore()
    for d in range(1, n_dev):
        pl.semaphore_signal(barrier, inc=1, device_id={"sp": lax.rem(me + d, n_dev)}, device_id_type=pl.DeviceIdType.MESH)
    pl.semaphore_wait(barrier, n_dev - 1)

    def exchange(src_of, dst_of, ex, bs):
        for d in range(1, n_dev):
            peer = lax.rem(me + d, n_dev)
            for b in bs:
                pltpu.make_async_remote_copy(
                    src_ref=src_of(peer, b), dst_ref=dst_of(me, b), send_sem=send_sem.at[ex], recv_sem=recv_sem.at[ex],
                    device_id={"sp": peer}, device_id_type=pl.DeviceIdType.MESH).start()
        for b in bs:
            pltpu.make_async_copy(src_of(me, b), dst_of(me, b), recv_sem.at[ex]).start()

    def exchange_wait(whole_dst, part_src, ex):
        pltpu.make_async_copy(whole_dst, whole_dst, recv_sem.at[ex]).wait()
        pltpu.make_async_copy(part_src, part_src, send_sem.at[ex]).wait()

    def blk(owner, b):
        return pl.ds(pl.multiple_of(b * seq + owner * tok, tok), tok)

    exchange(lambda p, b: x_hbm.at[p * n_seq + b], lambda p, b: h.at[blk(p, b)], 0, range(n_seq))
    for c in in_copies:
        c.start()

    chan[0:CONV, :] = conv_w[...].astype(F32)
    chan[CONV:CONV + 1, :] = conv_b[...].astype(F32).reshape(1, inner)
    chan[CONV + 1:CONV + 2, :] = dt_b[...].reshape(1, inner)
    for j in range(lanes):
        neg = -jnp.exp(a_log[:, j * 128:(j + 1) * 128]) * LOG2E
        for m in range(n_state // 8):
            a2[pl.ds(m * 8 * PITCH + j, 8, stride=PITCH), :] = neg[m * 8:(m + 1) * 8]

    def relayout(i, n_heads, unit0, k0):
        slot = lax.rem(i, STAGE)
        per = 32 // n_heads
        pitch = n_heads + 1
        stage_copy(wq, 0, slot).wait()

        @pl.loop(0, KB * per // 32)
        def _(g2):
            for m in range(2):
                g = g2 * 2 + m
                base_row = m * 16 * 33
                for r in range(16 // per):
                    val = stage[slot, g * (16 // per) + r].astype(F32)
                    for j in range(per):
                        delta[pl.ds(base_row + (r * per + j) * pitch, n_heads), :] = val[j * n_heads:(j + 1) * n_heads]
                ks = pl.ds(pl.multiple_of(k0 + g * 16, 16), 16)
                for hd in range(n_heads):
                    w = WN // 128
                    ring[unit0 + hd // w, ks, (hd % w) * 128:(hd % w + 1) * 128] = (
                        delta[pl.ds(base_row + hd, 16, stride=pitch), :].astype(BF16))

        stage_start(i + STAGE)

    @pl.loop(0, n_q)
    def _(i):
        relayout(i, heads, 0, i * KB)

    for m in range(2):
        @pl.loop(0, n_kv)
        def _(i, m=m):
            relayout(n_q + m * n_kv + i, kv_heads, (qdim + m * kv_heads * 128) // WN, i * KB * (32 // kv_heads))

    exchange_wait(h, h.at[pl.ds(0, rows - n_seq * tok)], 0)
    norm_rows(attn_g)

    def project(u):
        return jnp.dot(a[...], ring[u], preferred_element_type=F32).astype(BF16)

    n_qu = qdim // WN
    n_qkv = qkv.shape[1] // WN
    for u in list(range(n_qu, n_qkv)) + [0, 1]:
        qkv[:, u * WN:(u + 1) * WN] = project(u)
    for u in list(range(n_qu, n_qkv)) + [0, 1]:
        start(jnp.int32(u + SLOTS), u + SLOTS, u + SLOTS)

    qi = lax.broadcasted_iota(jnp.int32, (seq, seq), 0)
    ki = lax.broadcasted_iota(jnp.int32, (seq, seq), 1)
    causal = jnp.concatenate([qi >= ki] * groups, axis=0)

    def attend(kvh, unit):
        qcols = [pl.ds(pl.multiple_of((kvh * groups + i) * 128, 128), 128) for i in range(groups)]
        rss = [pl.ds(b * seq, seq) for b in range(n_seq)]
        scores = []
        for rs in rss:
            kk = qkv[rs, pl.ds(pl.multiple_of(qdim + kvh * 128, 128), 128)]
            qq = jnp.concatenate([qkv[rs, c] for c in qcols], axis=0)
            scores.append(lax.dot_general(qq, kk, (((1,), (1,)), ((), ())), preferred_element_type=F32))
        nxt = None if unit is None else project(unit)
        probs = []
        for s in scores:
            s = jnp.where(causal, s * 128 ** -0.5, -jnp.inf)
            e = jnp.exp(s - jnp.max(s, axis=-1, keepdims=True))
            probs.append((e * (1.0 / jnp.sum(e, axis=-1, keepdims=True))).astype(BF16))
        for rs, p in zip(rss, probs):
            vv = qkv[rs, pl.ds(pl.multiple_of(qdim + (kv_heads + kvh) * 128, 128), 128)]
            o = jnp.dot(p, vv, preferred_element_type=F32).astype(BF16)
            for i, c in enumerate(qcols):
                qkv[rs, c] = o[i * seq:(i + 1) * seq]
        return nxt

    @pl.loop(0, kv_heads // 2 - 1)
    def _(i):
        nxt = [attend(2 * i + m, 2 * i + 2 + m) for m in range(2)]
        for m in range(2):
            qkv[:, cols(2 * i + 2 + m)] = nxt[m]
        for m in range(2):
            start(2 * i + 2 + m + SLOTS, SLOTS + 2, SLOTS + n_qu - 1)

    for m in range(2):
        attend(jnp.int32(kv_heads - 2 + m), None)

    def wo_body(t, w0, w1):
        acc = jnp.dot(qkv[:, :half_q], w0[...], preferred_element_type=F32)
        acc += jnp.dot(qkv[:, half_q:qdim], w1[...], preferred_element_type=F32)
        h[:, cols(t)] = (h[:, cols(t)].astype(F32) + acc).astype(BF16)

    phase(u_wo, dim // WN, wo_body, 2)
    norm_rows(mlp_g)

    def gu_body(t, w0, w1):
        g = jnp.dot(a[...], w0[...], preferred_element_type=F32)
        u = jnp.dot(a[...], w1[...], preferred_element_type=F32)
        act[:, cols(t)] = (silu(g) * u).astype(BF16)

    phase(u_gu, ff // WN, gu_body, 2)

    def dn_body(t, *ws):
        acc = None
        for (s, n), w in zip(chunks(ff), ws):
            d = jnp.dot(act[:, s:s + n], w[...], preferred_element_type=F32)
            acc = d if acc is None else acc + d
        h[:, cols(t)] = (h[:, cols(t)].astype(F32) + acc).astype(BF16)

    phase(u_dn, dim // WN, dn_body)
    norm_rows(mamba_g)

    row_id = lax.broadcasted_iota(jnp.int32, (seq, 1), 0)

    def scatter(dst, r0, t, val):
        for j in range(WN // 128):
            for i in range(seq // 8):
                dst[pl.ds((r0 + i * 8) * PITCH + t * (WN // 128) + j, 8, stride=PITCH), :] = (
                    val[i * 8:(i + 1) * 8, j * 128:(j + 1) * 128])

    def wx_body(t, w):
        res = jnp.dot(a[...], w[...], preferred_element_type=F32).astype(BF16).astype(F32)
        for b in range(n_seq):
            xi = res[b * seq:(b + 1) * seq]
            acc = chan[4:5, cols(t)] + chan[CONV - 1:CONV, cols(t)] * xi
            for j in range(CONV - 1):
                back = CONV - 1 - j
                prev = jnp.where(row_id >= back, pltpu.roll(xi, back, axis=0), 0.0)
                acc += chan[j:j + 1, cols(t)] * prev
            c = silu(acc).astype(BF16)
            act[b * seq:(b + 1) * seq, cols(t)] = c
            scatter(xs, b * seq, t, c.astype(F32))

    phase(u_wx, inner // WN, wx_body, 2)

    in_copies[0].wait()
    r = lax.dot_general(act[:, :inner], wxp[...], (((1,), (1,)), ((), ())), preferred_element_type=F32)
    n_r = r.shape[1]
    gain_r = jnp.concatenate([dt_g[...].reshape(1, dt_rank), b_g[...].reshape(1, n_state), c_g[...].reshape(1, n_state)], axis=1)
    col = lax.broadcasted_iota(jnp.int32, (1, n_r), 1)
    sq = r * r

    def inv_of(mask, n):
        return lax.rsqrt(jnp.sum(jnp.where(mask, sq, 0.0), axis=-1, keepdims=True) * (1.0 / n) + EPS)

    m_dt = col < dt_rank
    m_b = (col >= dt_rank) & (col < dt_rank + n_state)
    m_c = col >= dt_rank + n_state
    inv = jnp.where(m_dt, inv_of(m_dt, dt_rank), jnp.where(m_b, inv_of(m_b, n_state), inv_of(m_c, n_state)))
    rn = r * inv * gain_r
    rn_ref[...] = rn
    dt_in = rn[:, :dt_rank].astype(BF16)
    act[:, inner:inner + dt_rank] = dt_in
    in_copies[1].wait()

    def wz_body(t, w):
        pre = jnp.dot(act[:, inner:inner + dt_rank], wdt[:, cols(t)], preferred_element_type=F32)
        qkv[:, cols(t)] = jnp.dot(a[...], w[...], preferred_element_type=F32).astype(BF16)
        pre = pre + chan[5:6, cols(t)]
        step = jnp.maximum(pre, 0.0) + jnp.log1p(jnp.exp(-jnp.abs(pre)))
        for b in range(n_seq):
            scatter(delta, b * seq, t, step[b * seq:(b + 1) * seq])

    phase(u_wz, inner // WN, wz_body, 2)

    def bcast(ref, idx):
        return jnp.broadcast_to(ref[pl.ds(idx, 1), :], (8, 128))

    toks = 8

    for b in range(n_seq):
        for n in range(n_state):
            for ref, c0 in ((bb, dt_rank + n), (cb, dt_rank + n_state + n)):
                ref[n * seq:(n + 1) * seq, :] = jnp.broadcast_to(rn_ref[b * seq:(b + 1) * seq, c0:c0 + 1], (seq, 128))

        @pl.loop(0, lanes // 8)
        def _(c, b=b):
            av = [a2[pl.ds(n * PITCH + c * 8, 8), :] for n in range(n_state)]
            dsk = dskip[pl.ds(pl.multiple_of(c * 8, 8), 8), :]

            def tokens(i, st):
                st = list(st)
                for k in range(toks):
                    r = i * toks + k
                    at = pl.ds((b * seq + r) * PITCH + c * 8, 8)
                    d = delta[at, :]
                    x = xs[at, :]
                    dx = d * x
                    terms = []
                    for n in range(n_state):
                        st[n] = jnp.exp2(d * av[n]) * st[n] + dx * bcast(bb, n * seq + r)
                        terms.append(st[n] * bcast(cb, n * seq + r))
                    terms.append(dsk * x)
                    while len(terms) > 1:
                        terms = [terms[m] + terms[m + 1] for m in range(0, len(terms) - 1, 2)] + (
                            [terms[-1]] if len(terms) % 2 else [])
                    delta[at, :] = terms[0]
                return tuple(st)

            st = tuple(jnp.zeros((8, 128), F32) for _ in range(n_state))
            lax.fori_loop(0, seq // toks, tokens, st)

        @pl.loop(0, seq // 16)
        def _(i, b=b):
            r0 = pl.multiple_of(b * seq + i * 16, 16)
            for j in range(lanes):
                y = jnp.concatenate([delta[pl.ds((r0 + 8 * m) * PITCH + j, 8, stride=PITCH), :] for m in range(2)], axis=0)
                z = qkv[pl.ds(r0, 16), j * 128:(j + 1) * 128].astype(F32)
                act[pl.ds(r0, 16), j * 128:(j + 1) * 128] = (y * silu(z)).astype(BF16)

        rs = pl.ds(b * seq, seq)
        @pl.loop(0, dim // WN)
        def _(t, b=b, rs=rs):
            views = []
            for j, (s, n) in enumerate(chunks(inner)):
                slot = lax.rem(u_out + 2 * t + j, SLOTS)
                if b == 0:
                    copy((wout, s, n), 0, slot).wait()
                views.append(jnp.dot(act[rs, s:s + n], ring[slot, :n], preferred_element_type=F32))
            a[rs, cols(t)] = (h[rs, cols(t)].astype(F32) + (views[0] + views[1])).astype(BF16)
            exchange(lambda p, b: a.at[blk(p, b), cols(t)], lambda p, b: out_ref.at[p * n_seq + b, :, cols(t)], 1, [b])

    exchange_wait(out_ref, a.at[pl.ds(0, rows - n_seq * tok)], 1)


def layer_pair(hidden, attn_norm, w_q, w_k, w_v, w_o, mlp_norm, w_gate, w_up, w_down, mamba_norm, w_in_x, w_in_z, conv_w, conv_b, w_xproj, dt_norm, b_norm, c_norm, w_dt, dt_bias, a_log, d_skip, w_out):
    n_batch, tok, dim = hidden.shape
    n_seq = n_batch // lax.axis_size("sp")
    rows = n_batch * tok
    inner, n_state = a_log.shape
    hbm = pl.BlockSpec(memory_space=pltpu.HBM)
    vm = pl.BlockSpec(memory_space=pltpu.VMEM)
    qkv_dim = (w_q.shape[1] + w_k.shape[1] + w_v.shape[1]) * 128
    return pl.pallas_call(
        block_kernel,
        out_shape=jax.ShapeDtypeStruct(hidden.shape, BF16),
        in_specs=[hbm] * 13 + [vm] * 11,
        out_specs=hbm,
        scratch_shapes=[
            pltpu.VMEM((SLOTS, dim, WN), BF16),
            pltpu.VMEM((STAGE, KB, 32, 128), BF16),
            pltpu.VMEM((rows, qkv_dim), BF16),
            pltpu.VMEM((rows, dim), BF16),
            pltpu.VMEM((rows, dim), BF16),
            pltpu.VMEM((rows, w_gate.shape[1]), BF16),
            pltpu.VMEM((rows * PITCH, 128), F32),
            pltpu.VMEM((rows * PITCH, 128), F32),
            pltpu.VMEM((128 * n_state, 128), F32),
            pltpu.VMEM((128 * n_state, 128), F32),
            pltpu.VMEM((w_xproj.shape[1], inner), BF16),
            pltpu.VMEM(w_dt.shape, BF16),
            pltpu.VMEM((n_state * PITCH, 128), F32),
            pltpu.VMEM((8, inner), F32),
            pltpu.VMEM((rows, w_xproj.shape[1]), F32),
            pltpu.SemaphoreType.DMA((SLOTS,)),
            pltpu.SemaphoreType.DMA((STAGE,)),
            pltpu.SemaphoreType.DMA((2,)),
            pltpu.SemaphoreType.DMA((2,)),
            pltpu.SemaphoreType.DMA((2,)),
        ],
        compiler_params=pltpu.CompilerParams(vmem_limit_bytes=67043328, collective_id=0, has_side_effects=True),
        name="block",
    )(hidden, w_q.reshape(-1, 32, 128), w_k.reshape(-1, 32, 128), w_v.reshape(-1, 32, 128), w_o.reshape(-1, dim),
      w_gate, w_up, w_down, w_in_x, w_in_z, w_xproj.T, w_dt, w_out, attn_norm, mlp_norm, mamba_norm, conv_w, conv_b,
      dt_norm, b_norm, c_norm, dt_bias, d_skip.reshape(-1, 128), a_log.T)


def solution(mesh):
    act_spec = P("dp", "sp", None)
    return jax.shard_map(
        layer_pair,
        mesh=mesh,
        in_specs=(act_spec,) + (P(),) * 23,
        out_specs=act_spec,
        check_vma=False,
    )
```

```python
import functools
import math
import jax
import jax.numpy as jnp
from jax import lax
from jax.experimental import pallas as pl
from jax.experimental.pallas import tpu as pltpu
from jax.sharding import PartitionSpec as P

EPS = 1e-6
CONV = 4
SLOTS = 12
STAGE = 6
KB = 64
WN = 512
PITCH = 41
F32 = jnp.float32
BF16 = jnp.bfloat16
LOG2E = math.log2(math.e)


def rms_scale(values, gain_vec):
    values_f = values.astype(F32)
    inv_rms = lax.rsqrt(jnp.mean(values_f * values_f, axis=-1, keepdims=True) + EPS)
    return values_f * inv_rms * gain_vec.astype(F32)


def silu(v):
    half = 0.5 * v
    return half + half * jnp.tanh(half)


def block_kernel(x_hbm, wq, wk, wv, wo, wg, wu, wd, wx, wz, wxp_hbm, wdt_hbm, wout,
                 attn_g, mlp_g, mamba_g, conv_w, conv_b, dt_g, b_g, c_g, dt_b, dskip, a_log, out_ref,
                 ring, stage, qkv, h, a, act, delta, xs, bb, cb, wxp, wdt, a2, chan, rn_ref,
                 ring_sem, stage_sem, in_sem, send_sem, recv_sem):
    rows, dim = h.shape
    n_seq, seq = 2, 128
    n_dev = x_hbm.shape[0] // n_seq
    tok = x_hbm.shape[1]
    me = lax.axis_index("sp")
    inner = wx.shape[1]
    ff = wg.shape[1]
    qdim = wo.shape[0]
    heads = qdim // 128
    kv_heads = (qkv.shape[1] - qdim) // 256
    groups = heads // kv_heads
    lanes = inner // 128
    n_state = a_log.shape[0]
    dt_rank = wdt.shape[0]
    unit = ring.shape[1]

    def chunks(total):
        return [(s, min(unit, total - s)) for s in range(0, total, unit)]

    def cols(t):
        return pl.ds(pl.multiple_of(t * WN, WN), WN)

    segs = []
    base = 0

    def add_seg(n_tiles, parts):
        nonlocal base
        first = base
        base = first + n_tiles * len(parts)
        segs.append((first, base, parts))
        return first

    half_q = qdim // 2
    u_qkv = add_seg(qkv.shape[1] // WN, [(None, 0, dim)])
    u_wo = add_seg(dim // WN, [(wo, 0, half_q), (wo, half_q, half_q)])
    u_gu = add_seg(ff // WN, [(wg, 0, dim), (wu, 0, dim)])
    u_dn = add_seg(dim // WN, [(wd, s, n) for s, n in chunks(ff)])
    u_wx = add_seg(inner // WN, [(wx, 0, dim)])
    u_wz = add_seg(inner // WN, [(wz, 0, dim)])
    u_out = add_seg(dim // WN, [(wout, s, n) for s, n in chunks(inner)])

    def copy(part, tile, slot):
        w, r0, nr = part
        return pltpu.make_async_copy(w.at[pl.ds(r0, nr), cols(tile)], ring.at[slot, pl.ds(0, nr)], ring_sem.at[slot])

    def start(u, lo, hi):
        for first, last, parts in segs:
            if hi < first or lo >= last or parts[0][0] is None:
                continue
            n = len(parts)
            for i, part in enumerate(parts):
                @pl.when((u >= first) & (u < last) & (lax.rem(u - first + n, n) == i))
                def _(part=part, first=first, n=n):
                    copy(part, lax.div(u - first, n), lax.rem(u, SLOTS)).start()

    def phase(first, n_tiles, body, per=1):
        parts = [s for s in segs if s[0] == first][0][2]
        n = len(parts)

        def group(t0, count):
            views = []
            for u in range(count * n):
                slot = lax.rem(first + t0 * n + u, SLOTS)
                part = parts[u % n]
                if part[0] is not None:
                    copy(part, 0, slot).wait()
                views.append(ring.at[slot, pl.ds(0, part[2])])
            for m in range(count):
                body(t0 + m, *views[m * n:(m + 1) * n])
            for u in range(count * n):
                start(first + t0 * n + u + SLOTS, first + SLOTS, first + SLOTS + n_tiles * n - 1)

        @pl.loop(0, n_tiles // per)
        def _(g):
            group(g * per, per)

        if n_tiles % per:
            group(jnp.int32(n_tiles - n_tiles % per), n_tiles % per)

    def norm_rows(g_ref):
        gain = g_ref[...].astype(F32).reshape(1, dim)

        @pl.loop(0, rows // 64)
        def _(i):
            for m in range(4):
                rs = pl.ds(pl.multiple_of(i * 64 + m * 16, 16), 16)
                hv = h[rs, :].astype(F32)
                inv = lax.rsqrt(jnp.mean(hv * hv, axis=-1, keepdims=True) + EPS)
                a[rs, :] = (h[rs, :].astype(F32) * inv * gain).astype(BF16)

    in_copies = [
        pltpu.make_async_copy(wxp_hbm, wxp, in_sem.at[0]),
        pltpu.make_async_copy(wdt_hbm, wdt, in_sem.at[1]),
    ]
    n_q = wq.shape[0] // KB
    n_kv = wk.shape[0] // KB

    def stage_copy(w, c, slot):
        return pltpu.make_async_copy(w.at[pl.ds(c * KB, KB)], stage.at[slot], stage_sem.at[slot])

    def stage_start(i):
        slot = lax.rem(i, STAGE)
        for w, lo, n in ((wq, 0, n_q), (wk, n_q, n_kv), (wv, n_q + n_kv, n_kv)):
            @pl.when((i >= lo) & (i < lo + n))
            def _(w=w, lo=lo):
                stage_copy(w, i - lo, slot).start()

    for i in range(STAGE):
        stage_start(jnp.int32(i))

    barrier = pltpu.get_barrier_semaphore()
    for d in range(1, n_dev):
        pl.semaphore_signal(barrier, inc=1, device_id={"sp": lax.rem(me + d, n_dev)}, device_id_type=pl.DeviceIdType.MESH)
    pl.semaphore_wait(barrier, n_dev - 1)

    def exchange(src_of, dst_of, ex, bs):
        for d in range(1, n_dev):
            peer = lax.rem(me + d, n_dev)
            for b in bs:
                pltpu.make_async_remote_copy(
                    src_ref=src_of(peer, b), dst_ref=dst_of(me, b), send_sem=send_sem.at[ex], recv_sem=recv_sem.at[ex],
                    device_id={"sp": peer}, device_id_type=pl.DeviceIdType.MESH).start()
        for b in bs:
            pltpu.make_async_copy(src_of(me, b), dst_of(me, b), recv_sem.at[ex]).start()

    def exchange_wait(whole_dst, part_src, ex):
        pltpu.make_async_copy(whole_dst, whole_dst, recv_sem.at[ex]).wait()
        pltpu.make_async_copy(part_src, part_src, send_sem.at[ex]).wait()

    def blk(owner, b):
        return pl.ds(pl.multiple_of(b * seq + owner * tok, tok), tok)

    exchange(lambda p, b: x_hbm.at[p * n_seq + b], lambda p, b: h.at[blk(p, b)], 0, range(n_seq))
    for c in in_copies:
        c.start()

    chan[0:CONV, :] = conv_w[...].astype(F32)
    chan[CONV:CONV + 1, :] = conv_b[...].astype(F32).reshape(1, inner)
    chan[CONV + 1:CONV + 2, :] = dt_b[...].reshape(1, inner)
    for j in range(lanes):
        neg = -jnp.exp(a_log[:, j * 128:(j + 1) * 128]) * LOG2E
        for m in range(n_state // 8):
            a2[pl.ds(m * 8 * PITCH + j, 8, stride=PITCH), :] = neg[m * 8:(m + 1) * 8]

    def relayout(i, n_heads, unit0, k0):
        slot = lax.rem(i, STAGE)
        per = 32 // n_heads
        pitch = n_heads + 1
        stage_copy(wq, 0, slot).wait()

        @pl.loop(0, KB * per // 32)
        def _(g2):
            for m in range(2):
                g = g2 * 2 + m
                base_row = m * 16 * 33
                for r in range(16 // per):
                    val = stage[slot, g * (16 // per) + r].astype(F32)
                    for j in range(per):
                        delta[pl.ds(base_row + (r * per + j) * pitch, n_heads), :] = val[j * n_heads:(j + 1) * n_heads]
                ks = pl.ds(pl.multiple_of(k0 + g * 16, 16), 16)
                for hd in range(n_heads):
                    w = WN // 128
                    ring[unit0 + hd // w, ks, (hd % w) * 128:(hd % w + 1) * 128] = (
                        delta[pl.ds(base_row + hd, 16, stride=pitch), :].astype(BF16))

        stage_start(i + STAGE)

    @pl.loop(0, n_q)
    def _(i):
        relayout(i, heads, 0, i * KB)

    for m in range(2):
        @pl.loop(0, n_kv)
        def _(i, m=m):
            relayout(n_q + m * n_kv + i, kv_heads, (qdim + m * kv_heads * 128) // WN, i * KB * (32 // kv_heads))

    exchange_wait(h, h.at[pl.ds(0, rows - n_seq * tok)], 0)
    norm_rows(attn_g)

    def project(u):
        return jnp.dot(a[...], ring[u], preferred_element_type=F32).astype(BF16)

    n_qu = qdim // WN
    n_qkv = qkv.shape[1] // WN
    for u in list(range(n_qu, n_qkv)) + [0, 1]:
        qkv[:, u * WN:(u + 1) * WN] = project(u)
    for u in list(range(n_qu, n_qkv)) + [0, 1]:
        start(jnp.int32(u + SLOTS), u + SLOTS, u + SLOTS)

    qi = lax.broadcasted_iota(jnp.int32, (seq, seq), 0)
    ki = lax.broadcasted_iota(jnp.int32, (seq, seq), 1)
    causal = jnp.concatenate([qi >= ki] * groups, axis=0)

    def attend(kvh, unit):
        qcols = [pl.ds(pl.multiple_of((kvh * groups + i) * 128, 128), 128) for i in range(groups)]
        rss = [pl.ds(b * seq, seq) for b in range(n_seq)]
        scores = []
        for rs in rss:
            kk = qkv[rs, pl.ds(pl.multiple_of(qdim + kvh * 128, 128), 128)]
            qq = jnp.concatenate([qkv[rs, c] for c in qcols], axis=0)
            scores.append(lax.dot_general(qq, kk, (((1,), (1,)), ((), ())), preferred_element_type=F32))
        nxt = None if unit is None else project(unit)
        probs = []
        for s in scores:
            s = jnp.where(causal, s * 128 ** -0.5, -jnp.inf)
            e = jnp.exp(s - jnp.max(s, axis=-1, keepdims=True))
            probs.append((e * (1.0 / jnp.sum(e, axis=-1, keepdims=True))).astype(BF16))
        for rs, p in zip(rss, probs):
            vv = qkv[rs, pl.ds(pl.multiple_of(qdim + (kv_heads + kvh) * 128, 128), 128)]
            o = jnp.dot(p, vv, preferred_element_type=F32).astype(BF16)
            for i, c in enumerate(qcols):
                qkv[rs, c] = o[i * seq:(i + 1) * seq]
        return nxt

    @pl.loop(0, kv_heads // 2 - 1)
    def _(i):
        nxt = [attend(2 * i + m, 2 * i + 2 + m) for m in range(2)]
        for m in range(2):
            qkv[:, cols(2 * i + 2 + m)] = nxt[m]
        for m in range(2):
            start(2 * i + 2 + m + SLOTS, SLOTS + 2, SLOTS + n_qu - 1)

    for m in range(2):
        attend(jnp.int32(kv_heads - 2 + m), None)

    def wo_body(t, w0, w1):
        acc = jnp.dot(qkv[:, :half_q], w0[...], preferred_element_type=F32)
        acc += jnp.dot(qkv[:, half_q:qdim], w1[...], preferred_element_type=F32)
        h[:, cols(t)] = (h[:, cols(t)].astype(F32) + acc).astype(BF16)

    phase(u_wo, dim // WN, wo_body, 2)
    norm_rows(mlp_g)

    def gu_body(t, w0, w1):
        g = jnp.dot(a[...], w0[...], preferred_element_type=F32)
        u = jnp.dot(a[...], w1[...], preferred_element_type=F32)
        act[:, cols(t)] = (silu(g) * u).astype(BF16)

    phase(u_gu, ff // WN, gu_body, 2)

    def dn_body(t, *ws):
        acc = None
        for (s, n), w in zip(chunks(ff), ws):
            d = jnp.dot(act[:, s:s + n], w[...], preferred_element_type=F32)
            acc = d if acc is None else acc + d
        h[:, cols(t)] = (h[:, cols(t)].astype(F32) + acc).astype(BF16)

    phase(u_dn, dim // WN, dn_body)
    norm_rows(mamba_g)

    row_id = lax.broadcasted_iota(jnp.int32, (seq, 1), 0)

    def scatter(dst, r0, t, val):
        for j in range(WN // 128):
            for i in range(seq // 8):
                dst[pl.ds((r0 + i * 8) * PITCH + t * (WN // 128) + j, 8, stride=PITCH), :] = (
                    val[i * 8:(i + 1) * 8, j * 128:(j + 1) * 128])

    def wx_body(t, w):
        res = jnp.dot(a[...], w[...], preferred_element_type=F32).astype(BF16).astype(F32)
        for b in range(n_seq):
            xi = res[b * seq:(b + 1) * seq]
            acc = chan[4:5, cols(t)] + chan[CONV - 1:CONV, cols(t)] * xi
            for j in range(CONV - 1):
                back = CONV - 1 - j
                prev = jnp.where(row_id >= back, pltpu.roll(xi, back, axis=0), 0.0)
                acc += chan[j:j + 1, cols(t)] * prev
            c = silu(acc).astype(BF16)
            act[b * seq:(b + 1) * seq, cols(t)] = c
            scatter(xs, b * seq, t, c.astype(F32))

    phase(u_wx, inner // WN, wx_body, 2)

    in_copies[0].wait()
    r = lax.dot_general(act[:, :inner], wxp[...], (((1,), (1,)), ((), ())), preferred_element_type=F32)
    n_r = r.shape[1]
    gain_r = jnp.concatenate([dt_g[...].reshape(1, dt_rank), b_g[...].reshape(1, n_state), c_g[...].reshape(1, n_state)], axis=1)
    col = lax.broadcasted_iota(jnp.int32, (1, n_r), 1)
    sq = r * r

    def inv_of(mask, n):
        return lax.rsqrt(jnp.sum(jnp.where(mask, sq, 0.0), axis=-1, keepdims=True) * (1.0 / n) + EPS)

    m_dt = col < dt_rank
    m_b = (col >= dt_rank) & (col < dt_rank + n_state)
    m_c = col >= dt_rank + n_state
    inv = jnp.where(m_dt, inv_of(m_dt, dt_rank), jnp.where(m_b, inv_of(m_b, n_state), inv_of(m_c, n_state)))
    rn = r * inv * gain_r
    rn_ref[...] = rn
    dt_in = rn[:, :dt_rank].astype(BF16)
    act[:, inner:inner + dt_rank] = dt_in
    in_copies[1].wait()

    def wz_body(t, w):
        pre = jnp.dot(act[:, inner:inner + dt_rank], wdt[:, cols(t)], preferred_element_type=F32)
        qkv[:, cols(t)] = jnp.dot(a[...], w[...], preferred_element_type=F32).astype(BF16)
        pre = pre + chan[5:6, cols(t)]
        step = jnp.maximum(pre, 0.0) + jnp.log1p(jnp.exp(-jnp.abs(pre)))
        for b in range(n_seq):
            scatter(delta, b * seq, t, step[b * seq:(b + 1) * seq])

    phase(u_wz, inner // WN, wz_body, 2)

    def bcast(ref, idx):
        return jnp.broadcast_to(ref[pl.ds(idx, 1), :], (8, 128))

    toks = 8

    for b in range(n_seq):
        for n in range(n_state):
            for ref, c0 in ((bb, dt_rank + n), (cb, dt_rank + n_state + n)):
                ref[n * seq:(n + 1) * seq, :] = jnp.broadcast_to(rn_ref[b * seq:(b + 1) * seq, c0:c0 + 1], (seq, 128))

        @pl.loop(0, lanes // 8)
        def _(c, b=b):
            av = [a2[pl.ds(n * PITCH + c * 8, 8), :] for n in range(n_state)]
            dsk = dskip[pl.ds(pl.multiple_of(c * 8, 8), 8), :]

            def tokens(i, st):
                st = list(st)
                for k in range(toks):
                    r = i * toks + k
                    at = pl.ds((b * seq + r) * PITCH + c * 8, 8)
                    d = delta[at, :]
                    x = xs[at, :]
                    dx = d * x
                    terms = []
                    for n in range(n_state):
                        st[n] = jnp.exp2(d * av[n]) * st[n] + dx * bcast(bb, n * seq + r)
                        terms.append(st[n] * bcast(cb, n * seq + r))
                    terms.append(dsk * x)
                    while len(terms) > 1:
                        terms = [terms[m] + terms[m + 1] for m in range(0, len(terms) - 1, 2)] + (
                            [terms[-1]] if len(terms) % 2 else [])
                    delta[at, :] = terms[0]
                return tuple(st)

            st = tuple(jnp.zeros((8, 128), F32) for _ in range(n_state))
            lax.fori_loop(0, seq // toks, tokens, st)

        @pl.loop(0, seq // 16)
        def _(i, b=b):
            r0 = pl.multiple_of(b * seq + i * 16, 16)
            for j in range(lanes):
                y = jnp.concatenate([delta[pl.ds((r0 + 8 * m) * PITCH + j, 8, stride=PITCH), :] for m in range(2)], axis=0)
                z = qkv[pl.ds(r0, 16), j * 128:(j + 1) * 128].astype(F32)
                act[pl.ds(r0, 16), j * 128:(j + 1) * 128] = (y * silu(z)).astype(BF16)

        rs = pl.ds(b * seq, seq)
        @pl.loop(0, dim // WN)
        def _(t, b=b, rs=rs):
            slots = [lax.rem(u_out + 2 * t + j, SLOTS) for j in range(2)]
            if b == 0:
                for (s, n), slot in zip(chunks(inner), slots):
                    copy((wout, s, n), 0, slot).wait()
            ds = [jnp.dot(act[rs, s:s + n], ring[slot, :n], preferred_element_type=F32)
                  for (s, n), slot in zip(chunks(inner), slots)]
            a[rs, cols(t)] = (h[rs, cols(t)].astype(F32) + (ds[0] + ds[1])).astype(BF16)
            exchange(lambda p, b: a.at[blk(p, b), cols(t)], lambda p, b: out_ref.at[p * n_seq + b, :, cols(t)], 1, [b])

    exchange_wait(out_ref, a.at[pl.ds(0, rows - n_seq * tok)], 1)


def layer_pair(hidden, attn_norm, w_q, w_k, w_v, w_o, mlp_norm, w_gate, w_up, w_down, mamba_norm, w_in_x, w_in_z, conv_w, conv_b, w_xproj, dt_norm, b_norm, c_norm, w_dt, dt_bias, a_log, d_skip, w_out):
    n_batch, tok, dim = hidden.shape
    n_seq = n_batch // lax.axis_size("sp")
    rows = n_batch * tok
    inner, n_state = a_log.shape
    hbm = pl.BlockSpec(memory_space=pltpu.HBM)
    vm = pl.BlockSpec(memory_space=pltpu.VMEM)
    qkv_dim = (w_q.shape[1] + w_k.shape[1] + w_v.shape[1]) * 128
    return pl.pallas_call(
        block_kernel,
        out_shape=jax.ShapeDtypeStruct(hidden.shape, BF16),
        in_specs=[hbm] * 13 + [vm] * 11,
        out_specs=hbm,
        scratch_shapes=[
            pltpu.VMEM((SLOTS, dim, WN), BF16),
            pltpu.VMEM((STAGE, KB, 32, 128), BF16),
            pltpu.VMEM((rows, qkv_dim), BF16),
            pltpu.VMEM((rows, dim), BF16),
            pltpu.VMEM((rows, dim), BF16),
            pltpu.VMEM((rows, w_gate.shape[1]), BF16),
            pltpu.VMEM((rows * PITCH, 128), F32),
            pltpu.VMEM((rows * PITCH, 128), F32),
            pltpu.VMEM((128 * n_state, 128), F32),
            pltpu.VMEM((128 * n_state, 128), F32),
            pltpu.VMEM((w_xproj.shape[1], inner), BF16),
            pltpu.VMEM(w_dt.shape, BF16),
            pltpu.VMEM((n_state * PITCH, 128), F32),
            pltpu.VMEM((8, inner), F32),
            pltpu.VMEM((rows, w_xproj.shape[1]), F32),
            pltpu.SemaphoreType.DMA((SLOTS,)),
            pltpu.SemaphoreType.DMA((STAGE,)),
            pltpu.SemaphoreType.DMA((2,)),
            pltpu.SemaphoreType.DMA((2,)),
            pltpu.SemaphoreType.DMA((2,)),
        ],
        compiler_params=pltpu.CompilerParams(vmem_limit_bytes=67043328, collective_id=0, has_side_effects=True),
        name="block",
    )(hidden, w_q.reshape(-1, 32, 128), w_k.reshape(-1, 32, 128), w_v.reshape(-1, 32, 128), w_o.reshape(-1, dim),
      w_gate, w_up, w_down, w_in_x, w_in_z, w_xproj.T, w_dt, w_out, attn_norm, mlp_norm, mamba_norm, conv_w, conv_b,
      dt_norm, b_norm, c_norm, dt_bias, d_skip.reshape(-1, 128), a_log.T)


def solution(mesh):
    act_spec = P("dp", "sp", None)
    return jax.shard_map(
        layer_pair,
        mesh=mesh,
        in_specs=(act_spec,) + (P(),) * 23,
        out_specs=act_spec,
        check_vma=False,
    )
```

```python
import functools
import math
import jax
import jax.numpy as jnp
from jax import lax
from jax.experimental import pallas as pl
from jax.experimental.pallas import tpu as pltpu
from jax.sharding import PartitionSpec as P

EPS = 1e-6
CONV = 4
SLOTS = 12
STAGE = 6
KB = 64
WN = 512
PITCH = 41
F32 = jnp.float32
BF16 = jnp.bfloat16
LOG2E = math.log2(math.e)


def rms_scale(values, gain_vec):
    values_f = values.astype(F32)
    inv_rms = lax.rsqrt(jnp.mean(values_f * values_f, axis=-1, keepdims=True) + EPS)
    return values_f * inv_rms * gain_vec.astype(F32)


def silu(v):
    half = 0.5 * v
    return half + half * jnp.tanh(half)


def block_kernel(x_hbm, wq, wk, wv, wo, wg, wu, wd, wx, wz, wxp_hbm, wdt_hbm, wout,
                 attn_g, mlp_g, mamba_g, conv_w, conv_b, dt_g, b_g, c_g, dt_b, dskip, a_log, out_ref,
                 ring, stage, qkv, h, a, act, delta, xs, bb, cb, wxp, wdt, a2, chan, rn_ref,
                 ring_sem, stage_sem, in_sem, send_sem, recv_sem):
    rows, dim = h.shape
    n_seq, seq = 2, 128
    n_dev = x_hbm.shape[0] // n_seq
    tok = x_hbm.shape[1]
    me = lax.axis_index("sp")
    inner = wx.shape[1]
    ff = wg.shape[1]
    qdim = wo.shape[0]
    heads = qdim // 128
    kv_heads = (qkv.shape[1] - qdim) // 256
    groups = heads // kv_heads
    lanes = inner // 128
    n_state = a_log.shape[0]
    dt_rank = wdt.shape[0]
    unit = ring.shape[1]

    def chunks(total):
        return [(s, min(unit, total - s)) for s in range(0, total, unit)]

    def cols(t):
        return pl.ds(pl.multiple_of(t * WN, WN), WN)

    segs = []
    base = 0

    def add_seg(n_tiles, parts):
        nonlocal base
        first = base
        base = first + n_tiles * len(parts)
        segs.append((first, base, parts))
        return first

    half_q = qdim // 2
    u_qkv = add_seg(qkv.shape[1] // WN, [(None, 0, dim)])
    u_wo = add_seg(dim // WN, [(wo, 0, half_q), (wo, half_q, half_q)])
    u_gu = add_seg(ff // WN, [(wg, 0, dim), (wu, 0, dim)])
    u_dn = add_seg(dim // WN, [(wd, s, n) for s, n in chunks(ff)])
    u_wx = add_seg(inner // WN, [(wx, 0, dim)])
    u_wz = add_seg(inner // WN, [(wz, 0, dim)])
    u_out = add_seg(dim // WN, [(wout, s, n) for s, n in chunks(inner)])

    def copy(part, tile, slot):
        w, r0, nr = part
        return pltpu.make_async_copy(w.at[pl.ds(r0, nr), cols(tile)], ring.at[slot, pl.ds(0, nr)], ring_sem.at[slot])

    def start(u, lo, hi):
        for first, last, parts in segs:
            if hi < first or lo >= last or parts[0][0] is None:
                continue
            n = len(parts)
            for i, part in enumerate(parts):
                @pl.when((u >= first) & (u < last) & (lax.rem(u - first + n, n) == i))
                def _(part=part, first=first, n=n):
                    copy(part, lax.div(u - first, n), lax.rem(u, SLOTS)).start()

    def phase(first, n_tiles, body, per=1):
        parts = [s for s in segs if s[0] == first][0][2]
        n = len(parts)

        def group(t0, count):
            views = []
            for u in range(count * n):
                slot = lax.rem(first + t0 * n + u, SLOTS)
                part = parts[u % n]
                if part[0] is not None:
                    copy(part, 0, slot).wait()
                views.append(ring.at[slot, pl.ds(0, part[2])])
            for m in range(count):
                body(t0 + m, *views[m * n:(m + 1) * n], **({'parity': m % 2} if body.__name__ == 'wx_body' else {}))
            for u in range(count * n):
                start(first + t0 * n + u + SLOTS, first + SLOTS, first + SLOTS + n_tiles * n - 1)

        @pl.loop(0, n_tiles // per)
        def _(g):
            group(g * per, per)

        if n_tiles % per:
            group(jnp.int32(n_tiles - n_tiles % per), n_tiles % per)

    def norm_rows(g_ref):
        gain = g_ref[...].astype(F32).reshape(1, dim)

        @pl.loop(0, rows // 64)
        def _(i):
            for m in range(4):
                rs = pl.ds(pl.multiple_of(i * 64 + m * 16, 16), 16)
                hv = h[rs, :].astype(F32)
                inv = lax.rsqrt(jnp.mean(hv * hv, axis=-1, keepdims=True) + EPS)
                a[rs, :] = (h[rs, :].astype(F32) * inv * gain).astype(BF16)

    in_copies = [
        pltpu.make_async_copy(wxp_hbm, wxp, in_sem.at[0]),
        pltpu.make_async_copy(wdt_hbm, wdt, in_sem.at[1]),
    ]
    n_q = wq.shape[0] // KB
    n_kv = wk.shape[0] // KB

    def stage_copy(w, c, slot):
        return pltpu.make_async_copy(w.at[pl.ds(c * KB, KB)], stage.at[slot], stage_sem.at[slot])

    def stage_start(i):
        slot = lax.rem(i, STAGE)
        for w, lo, n in ((wq, 0, n_q), (wk, n_q, n_kv), (wv, n_q + n_kv, n_kv)):
            @pl.when((i >= lo) & (i < lo + n))
            def _(w=w, lo=lo):
                stage_copy(w, i - lo, slot).start()

    for i in range(STAGE):
        stage_start(jnp.int32(i))

    barrier = pltpu.get_barrier_semaphore()
    for d in range(1, n_dev):
        pl.semaphore_signal(barrier, inc=1, device_id={"sp": lax.rem(me + d, n_dev)}, device_id_type=pl.DeviceIdType.MESH)
    pl.semaphore_wait(barrier, n_dev - 1)

    def exchange(src_of, dst_of, ex, bs):
        for d in range(1, n_dev):
            peer = lax.rem(me + d, n_dev)
            for b in bs:
                pltpu.make_async_remote_copy(
                    src_ref=src_of(peer, b), dst_ref=dst_of(me, b), send_sem=send_sem.at[ex], recv_sem=recv_sem.at[ex],
                    device_id={"sp": peer}, device_id_type=pl.DeviceIdType.MESH).start()
        for b in bs:
            pltpu.make_async_copy(src_of(me, b), dst_of(me, b), recv_sem.at[ex]).start()

    def exchange_wait(whole_dst, part_src, ex):
        pltpu.make_async_copy(whole_dst, whole_dst, recv_sem.at[ex]).wait()
        pltpu.make_async_copy(part_src, part_src, send_sem.at[ex]).wait()

    def blk(owner, b):
        return pl.ds(pl.multiple_of(b * seq + owner * tok, tok), tok)

    exchange(lambda p, b: x_hbm.at[p * n_seq + b], lambda p, b: h.at[blk(p, b)], 0, range(n_seq))
    for c in in_copies:
        c.start()

    chan[0:CONV, :] = conv_w[...].astype(F32)
    chan[CONV:CONV + 1, :] = conv_b[...].astype(F32).reshape(1, inner)
    chan[CONV + 1:CONV + 2, :] = dt_b[...].reshape(1, inner)
    for j in range(lanes):
        neg = -jnp.exp(a_log[:, j * 128:(j + 1) * 128]) * LOG2E
        for m in range(n_state // 8):
            a2[pl.ds(m * 8 * PITCH + j, 8, stride=PITCH), :] = neg[m * 8:(m + 1) * 8]

    def relayout(i, n_heads, unit0, k0):
        slot = lax.rem(i, STAGE)
        per = 32 // n_heads
        pitch = n_heads + 1
        stage_copy(wq, 0, slot).wait()

        @pl.loop(0, KB * per // 32)
        def _(g2):
            for m in range(2):
                g = g2 * 2 + m
                base_row = m * 16 * 33
                for r in range(16 // per):
                    val = stage[slot, g * (16 // per) + r].astype(F32)
                    for j in range(per):
                        delta[pl.ds(base_row + (r * per + j) * pitch, n_heads), :] = val[j * n_heads:(j + 1) * n_heads]
                ks = pl.ds(pl.multiple_of(k0 + g * 16, 16), 16)
                for hd in range(n_heads):
                    w = WN // 128
                    ring[unit0 + hd // w, ks, (hd % w) * 128:(hd % w + 1) * 128] = (
                        delta[pl.ds(base_row + hd, 16, stride=pitch), :].astype(BF16))

        stage_start(i + STAGE)

    @pl.loop(0, n_q)
    def _(i):
        relayout(i, heads, 0, i * KB)

    for m in range(2):
        @pl.loop(0, n_kv)
        def _(i, m=m):
            relayout(n_q + m * n_kv + i, kv_heads, (qdim + m * kv_heads * 128) // WN, i * KB * (32 // kv_heads))

    exchange_wait(h, h.at[pl.ds(0, rows - n_seq * tok)], 0)
    norm_rows(attn_g)

    def project(u):
        return jnp.dot(a[...], ring[u], preferred_element_type=F32).astype(BF16)

    n_qu = qdim // WN
    n_qkv = qkv.shape[1] // WN
    for u in list(range(n_qu, n_qkv)) + [0, 1]:
        qkv[:, u * WN:(u + 1) * WN] = project(u)
    for u in list(range(n_qu, n_qkv)) + [0, 1]:
        start(jnp.int32(u + SLOTS), u + SLOTS, u + SLOTS)

    qi = lax.broadcasted_iota(jnp.int32, (seq, seq), 0)
    ki = lax.broadcasted_iota(jnp.int32, (seq, seq), 1)
    causal = jnp.concatenate([qi >= ki] * groups, axis=0)

    def attend(kvh, unit):
        qcols = [pl.ds(pl.multiple_of((kvh * groups + i) * 128, 128), 128) for i in range(groups)]
        rss = [pl.ds(b * seq, seq) for b in range(n_seq)]
        scores = []
        for rs in rss:
            kk = qkv[rs, pl.ds(pl.multiple_of(qdim + kvh * 128, 128), 128)]
            qq = jnp.concatenate([qkv[rs, c] for c in qcols], axis=0)
            scores.append(lax.dot_general(qq, kk, (((1,), (1,)), ((), ())), preferred_element_type=F32))
        nxt = None if unit is None else project(unit)
        probs = []
        for s in scores:
            s = jnp.where(causal, s * 128 ** -0.5, -jnp.inf)
            e = jnp.exp(s - jnp.max(s, axis=-1, keepdims=True))
            probs.append((e * (1.0 / jnp.sum(e, axis=-1, keepdims=True))).astype(BF16))
        for rs, p in zip(rss, probs):
            vv = qkv[rs, pl.ds(pl.multiple_of(qdim + (kv_heads + kvh) * 128, 128), 128)]
            o = jnp.dot(p, vv, preferred_element_type=F32).astype(BF16)
            for i, c in enumerate(qcols):
                qkv[rs, c] = o[i * seq:(i + 1) * seq]
        return nxt

    @pl.loop(0, kv_heads // 2 - 1)
    def _(i):
        nxt = [attend(2 * i + m, 2 * i + 2 + m) for m in range(2)]
        for m in range(2):
            qkv[:, cols(2 * i + 2 + m)] = nxt[m]
        for m in range(2):
            start(2 * i + 2 + m + SLOTS, SLOTS + 2, SLOTS + n_qu - 1)

    for m in range(2):
        attend(jnp.int32(kv_heads - 2 + m), None)

    def wo_body(t, w0, w1):
        acc = jnp.dot(qkv[:, :half_q], w0[...], preferred_element_type=F32)
        acc += jnp.dot(qkv[:, half_q:qdim], w1[...], preferred_element_type=F32)
        h[:, cols(t)] = (h[:, cols(t)].astype(F32) + acc).astype(BF16)

    phase(u_wo, dim // WN, wo_body, 2)
    norm_rows(mlp_g)

    def gu_body(t, w0, w1):
        g = jnp.dot(a[...], w0[...], preferred_element_type=F32)
        u = jnp.dot(a[...], w1[...], preferred_element_type=F32)
        act[:, cols(t)] = (silu(g) * u).astype(BF16)

    phase(u_gu, ff // WN, gu_body, 2)

    def dn_body(t, *ws):
        acc = None
        for (s, n), w in zip(chunks(ff), ws):
            d = jnp.dot(act[:, s:s + n], w[...], preferred_element_type=F32)
            acc = d if acc is None else acc + d
        h[:, cols(t)] = (h[:, cols(t)].astype(F32) + acc).astype(BF16)

    phase(u_dn, dim // WN, dn_body)
    norm_rows(mamba_g)

    row_id = lax.broadcasted_iota(jnp.int32, (seq, 1), 0)

    def scatter(dst, r0, t, val):
        for j in range(WN // 128):
            for i in range(seq // 8):
                dst[pl.ds((r0 + i * 8) * PITCH + t * (WN // 128) + j, 8, stride=PITCH), :] = (
                    val[i * 8:(i + 1) * 8, j * 128:(j + 1) * 128])

    conv_pitch = seq + 8
    for k in range(2 * n_seq * (WN // 128)):
        delta[k * conv_pitch:k * conv_pitch + 8, :] = jnp.zeros((8, 128), F32)

    def wx_body(t, w, parity=0):
        res = jnp.dot(a[...], w[...], preferred_element_type=F32).astype(BF16).astype(F32)
        for b in range(n_seq):
            for j in range(WN // 128):
                top = ((parity * n_seq + b) * (WN // 128) + j) * conv_pitch + 8
                cj = pl.ds(pl.multiple_of(t * WN, WN) + j * 128, 128)
                xi = res[b * seq:(b + 1) * seq, j * 128:(j + 1) * 128]
                delta[top:top + seq, :] = xi
                acc = chan[4:5, cj] + chan[CONV - 1:CONV, cj] * xi
                for k in range(CONV - 1):
                    back = CONV - 1 - k
                    acc += chan[k:k + 1, cj] * delta[top - back:top - back + seq, :]
                c = silu(acc).astype(BF16)
                act[b * seq:(b + 1) * seq, cj] = c
                cf = c.astype(F32)
                for i in range(seq // 8):
                    xs[pl.ds((b * seq + i * 8) * PITCH + t * (WN // 128) + j, 8, stride=PITCH), :] = cf[i * 8:(i + 1) * 8]

    phase(u_wx, inner // WN, wx_body, 2)

    in_copies[0].wait()
    r = lax.dot_general(act[:, :inner], wxp[...], (((1,), (1,)), ((), ())), preferred_element_type=F32)
    n_r = r.shape[1]
    gain_r = jnp.concatenate([dt_g[...].reshape(1, dt_rank), b_g[...].reshape(1, n_state), c_g[...].reshape(1, n_state)], axis=1)
    col = lax.broadcasted_iota(jnp.int32, (1, n_r), 1)
    sq = r * r

    def inv_of(mask, n):
        return lax.rsqrt(jnp.sum(jnp.where(mask, sq, 0.0), axis=-1, keepdims=True) * (1.0 / n) + EPS)

    m_dt = col < dt_rank
    m_b = (col >= dt_rank) & (col < dt_rank + n_state)
    m_c = col >= dt_rank + n_state
    inv = jnp.where(m_dt, inv_of(m_dt, dt_rank), jnp.where(m_b, inv_of(m_b, n_state), inv_of(m_c, n_state)))
    rn = r * inv * gain_r
    rn_ref[...] = rn
    dt_in = rn[:, :dt_rank].astype(BF16)
    act[:, inner:inner + dt_rank] = dt_in
    in_copies[1].wait()

    def wz_body(t, w):
        pre = jnp.dot(act[:, inner:inner + dt_rank], wdt[:, cols(t)], preferred_element_type=F32)
        qkv[:, cols(t)] = jnp.dot(a[...], w[...], preferred_element_type=F32).astype(BF16)
        pre = pre + chan[5:6, cols(t)]
        step = jnp.maximum(pre, 0.0) + jnp.log1p(jnp.exp(-jnp.abs(pre)))
        for b in range(n_seq):
            scatter(delta, b * seq, t, step[b * seq:(b + 1) * seq])

    phase(u_wz, inner // WN, wz_body, 2)

    def bcast(ref, idx):
        return jnp.broadcast_to(ref[pl.ds(idx, 1), :], (8, 128))

    toks = 8

    for b in range(n_seq):
        for n in range(n_state):
            for ref, c0 in ((bb, dt_rank + n), (cb, dt_rank + n_state + n)):
                ref[n * seq:(n + 1) * seq, :] = jnp.broadcast_to(rn_ref[b * seq:(b + 1) * seq, c0:c0 + 1], (seq, 128))

        @pl.loop(0, lanes // 8)
        def _(c, b=b):
            av = [a2[pl.ds(n * PITCH + c * 8, 8), :] for n in range(n_state)]
            dsk = dskip[pl.ds(pl.multiple_of(c * 8, 8), 8), :]

            def tokens(i, st):
                st = list(st)
                for k in range(toks):
                    r = i * toks + k
                    at = pl.ds((b * seq + r) * PITCH + c * 8, 8)
                    d = delta[at, :]
                    x = xs[at, :]
                    dx = d * x
                    terms = []
                    for n in range(n_state):
                        st[n] = jnp.exp2(d * av[n]) * st[n] + dx * bcast(bb, n * seq + r)
                        terms.append(st[n] * bcast(cb, n * seq + r))
                    terms.append(dsk * x)
                    while len(terms) > 1:
                        terms = [terms[m] + terms[m + 1] for m in range(0, len(terms) - 1, 2)] + (
                            [terms[-1]] if len(terms) % 2 else [])
                    delta[at, :] = terms[0]
                return tuple(st)

            st = tuple(jnp.zeros((8, 128), F32) for _ in range(n_state))
            lax.fori_loop(0, seq // toks, tokens, st)

        @pl.loop(0, seq // 16)
        def _(i, b=b):
            r0 = pl.multiple_of(b * seq + i * 16, 16)
            for j in range(lanes):
                y = jnp.concatenate([delta[pl.ds((r0 + 8 * m) * PITCH + j, 8, stride=PITCH), :] for m in range(2)], axis=0)
                z = qkv[pl.ds(r0, 16), j * 128:(j + 1) * 128].astype(F32)
                act[pl.ds(r0, 16), j * 128:(j + 1) * 128] = (y * silu(z)).astype(BF16)

        rs = pl.ds(b * seq, seq)
        n_t = dim // WN
        if b == 0:
            for t in range(n_t):
                for j, (s, n) in enumerate(chunks(inner)):
                    copy((wout, s, n), 0, (u_out + 2 * t + j) % SLOTS).wait()
        for t in range(n_t):
            ct = pl.ds(t * WN, WN)
            ds = [jnp.dot(act[rs, s:s + n], ring[(u_out + 2 * t + j) % SLOTS, :n], preferred_element_type=F32)
                  for j, (s, n) in enumerate(chunks(inner))]
            a[rs, ct] = (h[rs, ct].astype(F32) + (ds[0] + ds[1])).astype(BF16)
            exchange(lambda p, b: a.at[blk(p, b), ct], lambda p, b: out_ref.at[p * n_seq + b, :, ct], 1, [b])

    exchange_wait(out_ref, a.at[pl.ds(0, rows - n_seq * tok)], 1)


def layer_pair(hidden, attn_norm, w_q, w_k, w_v, w_o, mlp_norm, w_gate, w_up, w_down, mamba_norm, w_in_x, w_in_z, conv_w, conv_b, w_xproj, dt_norm, b_norm, c_norm, w_dt, dt_bias, a_log, d_skip, w_out):
    n_batch, tok, dim = hidden.shape
    n_seq = n_batch // lax.axis_size("sp")
    rows = n_batch * tok
    inner, n_state = a_log.shape
    hbm = pl.BlockSpec(memory_space=pltpu.HBM)
    vm = pl.BlockSpec(memory_space=pltpu.VMEM)
    qkv_dim = (w_q.shape[1] + w_k.shape[1] + w_v.shape[1]) * 128
    return pl.pallas_call(
        block_kernel,
        out_shape=jax.ShapeDtypeStruct(hidden.shape, BF16),
        in_specs=[hbm] * 13 + [vm] * 11,
        out_specs=hbm,
        scratch_shapes=[
            pltpu.VMEM((SLOTS, dim, WN), BF16),
            pltpu.VMEM((STAGE, KB, 32, 128), BF16),
            pltpu.VMEM((rows, qkv_dim), BF16),
            pltpu.VMEM((rows, dim), BF16),
            pltpu.VMEM((rows, dim), BF16),
            pltpu.VMEM((rows, w_gate.shape[1]), BF16),
            pltpu.VMEM((rows * PITCH, 128), F32),
            pltpu.VMEM((rows * PITCH, 128), F32),
            pltpu.VMEM((128 * n_state, 128), F32),
            pltpu.VMEM((128 * n_state, 128), F32),
            pltpu.VMEM((w_xproj.shape[1], inner), BF16),
            pltpu.VMEM(w_dt.shape, BF16),
            pltpu.VMEM((n_state * PITCH, 128), F32),
            pltpu.VMEM((8, inner), F32),
            pltpu.VMEM((rows, w_xproj.shape[1]), F32),
            pltpu.SemaphoreType.DMA((SLOTS,)),
            pltpu.SemaphoreType.DMA((STAGE,)),
            pltpu.SemaphoreType.DMA((2,)),
            pltpu.SemaphoreType.DMA((2,)),
            pltpu.SemaphoreType.DMA((2,)),
        ],
        compiler_params=pltpu.CompilerParams(vmem_limit_bytes=67043328, collective_id=0, has_side_effects=True),
        name="block",
    )(hidden, w_q.reshape(-1, 32, 128), w_k.reshape(-1, 32, 128), w_v.reshape(-1, 32, 128), w_o.reshape(-1, dim),
      w_gate, w_up, w_down, w_in_x, w_in_z, w_xproj.T, w_dt, w_out, attn_norm, mlp_norm, mamba_norm, conv_w, conv_b,
      dt_norm, b_norm, c_norm, dt_bias, d_skip.reshape(-1, 128), a_log.T)


def solution(mesh):
    act_spec = P("dp", "sp", None)
    return jax.shard_map(
        layer_pair,
        mesh=mesh,
        in_specs=(act_spec,) + (P(),) * 23,
        out_specs=act_spec,
        check_vma=False,
    )
```

```python
import functools
import math
import jax
import jax.numpy as jnp
from jax import lax
from jax.experimental import pallas as pl
from jax.experimental.pallas import tpu as pltpu
from jax.sharding import PartitionSpec as P

EPS = 1e-6
CONV = 4
SLOTS = 12
STAGE = 6
KB = 64
WN = 512
PITCH = 41
F32 = jnp.float32
BF16 = jnp.bfloat16
LOG2E = math.log2(math.e)


def rms_scale(values, gain_vec):
    values_f = values.astype(F32)
    inv_rms = lax.rsqrt(jnp.mean(values_f * values_f, axis=-1, keepdims=True) + EPS)
    return values_f * inv_rms * gain_vec.astype(F32)


def silu(v):
    half = 0.5 * v
    return half + half * jnp.tanh(half)


def block_kernel(x_hbm, wq, wk, wv, wo, wg, wu, wd, wx, wz, wxp_hbm, wdt_hbm, wout,
                 attn_g, mlp_g, mamba_g, conv_w, conv_b, dt_g, b_g, c_g, dt_b, dskip, a_log, out_ref,
                 ring, stage, qkv, h, a, act, delta, xs, bb, cb, wxp, wdt, a2, chan, rn_ref,
                 ring_sem, stage_sem, in_sem, send_sem, recv_sem):
    rows, dim = h.shape
    n_seq, seq = 2, 128
    n_dev = x_hbm.shape[0] // n_seq
    tok = x_hbm.shape[1]
    me = lax.axis_index("sp")
    inner = wx.shape[1]
    ff = wg.shape[1]
    qdim = wo.shape[0]
    heads = qdim // 128
    kv_heads = (qkv.shape[1] - qdim) // 256
    groups = heads // kv_heads
    lanes = inner // 128
    n_state = a_log.shape[0]
    dt_rank = wdt.shape[0]
    unit = ring.shape[1]

    def chunks(total):
        return [(s, min(unit, total - s)) for s in range(0, total, unit)]

    def cols(t):
        return pl.ds(pl.multiple_of(t * WN, WN), WN)

    segs = []
    base = 0

    def add_seg(n_tiles, parts):
        nonlocal base
        first = base
        base = first + n_tiles * len(parts)
        segs.append((first, base, parts))
        return first

    half_q = qdim // 2
    u_qkv = add_seg(qkv.shape[1] // WN, [(None, 0, dim)])
    u_wo = add_seg(dim // WN, [(wo, 0, half_q), (wo, half_q, half_q)])
    u_gu = add_seg(ff // WN, [(wg, 0, dim), (wu, 0, dim)])
    u_dn = add_seg(dim // WN, [(wd, s, n) for s, n in chunks(ff)])
    u_wx = add_seg(inner // WN, [(wx, 0, dim)])
    u_wz = add_seg(inner // WN, [(wz, 0, dim)])
    u_out = add_seg(dim // WN, [(wout, s, n) for s, n in chunks(inner)])

    def copy(part, tile, slot):
        w, r0, nr = part
        return pltpu.make_async_copy(w.at[pl.ds(r0, nr), cols(tile)], ring.at[slot, pl.ds(0, nr)], ring_sem.at[slot])

    def start(u, lo, hi):
        for first, last, parts in segs:
            if hi < first or lo >= last or parts[0][0] is None:
                continue
            n = len(parts)
            for i, part in enumerate(parts):
                @pl.when((u >= first) & (u < last) & (lax.rem(u - first + n, n) == i))
                def _(part=part, first=first, n=n):
                    copy(part, lax.div(u - first, n), lax.rem(u, SLOTS)).start()

    def phase(first, n_tiles, body, per=1):
        parts = [s for s in segs if s[0] == first][0][2]
        n = len(parts)

        def group(t0, count):
            views = []
            for u in range(count * n):
                slot = lax.rem(first + t0 * n + u, SLOTS)
                part = parts[u % n]
                if part[0] is not None:
                    copy(part, 0, slot).wait()
                views.append(ring.at[slot, pl.ds(0, part[2])])
            for m in range(count):
                body(t0 + m, *views[m * n:(m + 1) * n], **({'parity': m % 2} if body.__name__ == 'wx_body' else {}))
            for u in range(count * n):
                start(first + t0 * n + u + SLOTS, first + SLOTS, first + SLOTS + n_tiles * n - 1)

        @pl.loop(0, n_tiles // per)
        def _(g):
            group(g * per, per)

        if n_tiles % per:
            group(jnp.int32(n_tiles - n_tiles % per), n_tiles % per)

    def norm_rows(g_ref):
        gain = g_ref[...].astype(F32).reshape(1, dim)

        @pl.loop(0, rows // 64)
        def _(i):
            for m in range(4):
                rs = pl.ds(pl.multiple_of(i * 64 + m * 16, 16), 16)
                hv = h[rs, :].astype(F32)
                inv = lax.rsqrt(jnp.mean(hv * hv, axis=-1, keepdims=True) + EPS)
                a[rs, :] = (h[rs, :].astype(F32) * inv * gain).astype(BF16)

    in_copies = [
        pltpu.make_async_copy(wxp_hbm, wxp, in_sem.at[0]),
        pltpu.make_async_copy(wdt_hbm, wdt, in_sem.at[1]),
    ]
    n_q = wq.shape[0] // KB
    n_kv = wk.shape[0] // KB

    def stage_copy(w, c, slot):
        return pltpu.make_async_copy(w.at[pl.ds(c * KB, KB)], stage.at[slot], stage_sem.at[slot])

    def stage_start(i):
        slot = lax.rem(i, STAGE)
        for w, lo, n in ((wq, 0, n_q), (wk, n_q, n_kv), (wv, n_q + n_kv, n_kv)):
            @pl.when((i >= lo) & (i < lo + n))
            def _(w=w, lo=lo):
                stage_copy(w, i - lo, slot).start()

    for i in range(STAGE):
        stage_start(jnp.int32(i))

    barrier = pltpu.get_barrier_semaphore()
    for d in range(1, n_dev):
        pl.semaphore_signal(barrier, inc=1, device_id={"sp": lax.rem(me + d, n_dev)}, device_id_type=pl.DeviceIdType.MESH)
    pl.semaphore_wait(barrier, n_dev - 1)

    def exchange(src_of, dst_of, ex, bs):
        for d in range(1, n_dev):
            peer = lax.rem(me + d, n_dev)
            for b in bs:
                pltpu.make_async_remote_copy(
                    src_ref=src_of(peer, b), dst_ref=dst_of(me, b), send_sem=send_sem.at[ex], recv_sem=recv_sem.at[ex],
                    device_id={"sp": peer}, device_id_type=pl.DeviceIdType.MESH).start()
        for b in bs:
            pltpu.make_async_copy(src_of(me, b), dst_of(me, b), recv_sem.at[ex]).start()

    def exchange_wait(whole_dst, part_src, ex):
        pltpu.make_async_copy(whole_dst, whole_dst, recv_sem.at[ex]).wait()
        pltpu.make_async_copy(part_src, part_src, send_sem.at[ex]).wait()

    def blk(owner, b):
        return pl.ds(pl.multiple_of(b * seq + owner * tok, tok), tok)

    exchange(lambda p, b: x_hbm.at[p * n_seq + b], lambda p, b: h.at[blk(p, b)], 0, range(n_seq))
    for c in in_copies:
        c.start()

    chan[0:CONV, :] = conv_w[...].astype(F32)
    chan[CONV:CONV + 1, :] = conv_b[...].astype(F32).reshape(1, inner)
    chan[CONV + 1:CONV + 2, :] = dt_b[...].reshape(1, inner)
    for j in range(lanes):
        neg = -jnp.exp(a_log[:, j * 128:(j + 1) * 128]) * LOG2E
        for m in range(n_state // 8):
            a2[pl.ds(m * 8 * PITCH + j, 8, stride=PITCH), :] = neg[m * 8:(m + 1) * 8]

    def relayout(i, n_heads, unit0, k0):
        slot = lax.rem(i, STAGE)
        per = 32 // n_heads
        pitch = n_heads + 1
        stage_copy(wq, 0, slot).wait()

        @pl.loop(0, KB * per // 32)
        def _(g2):
            for m in range(2):
                g = g2 * 2 + m
                base_row = m * 16 * 33
                for r in range(16 // per):
                    val = stage[slot, g * (16 // per) + r].astype(F32)
                    for j in range(per):
                        delta[pl.ds(base_row + (r * per + j) * pitch, n_heads), :] = val[j * n_heads:(j + 1) * n_heads]
                ks = pl.ds(pl.multiple_of(k0 + g * 16, 16), 16)
                for hd in range(n_heads):
                    w = WN // 128
                    ring[unit0 + hd // w, ks, (hd % w) * 128:(hd % w + 1) * 128] = (
                        delta[pl.ds(base_row + hd, 16, stride=pitch), :].astype(BF16))

        stage_start(i + STAGE)

    @pl.loop(0, n_q)
    def _(i):
        relayout(i, heads, 0, i * KB)

    for m in range(2):
        @pl.loop(0, n_kv)
        def _(i, m=m):
            relayout(n_q + m * n_kv + i, kv_heads, (qdim + m * kv_heads * 128) // WN, i * KB * (32 // kv_heads))

    exchange_wait(h, h.at[pl.ds(0, rows - n_seq * tok)], 0)
    norm_rows(attn_g)

    def project(u):
        return jnp.dot(a[...], ring[u], preferred_element_type=F32).astype(BF16)

    n_qu = qdim // WN
    n_qkv = qkv.shape[1] // WN
    for u in list(range(n_qu, n_qkv)) + [0, 1]:
        qkv[:, u * WN:(u + 1) * WN] = project(u)
    for u in list(range(n_qu, n_qkv)) + [0, 1]:
        start(jnp.int32(u + SLOTS), u + SLOTS, u + SLOTS)

    qi = lax.broadcasted_iota(jnp.int32, (seq, seq), 0)
    ki = lax.broadcasted_iota(jnp.int32, (seq, seq), 1)
    causal = jnp.concatenate([qi >= ki] * groups, axis=0)

    def attend(kvh, unit):
        qcols = [pl.ds(pl.multiple_of((kvh * groups + i) * 128, 128), 128) for i in range(groups)]
        rss = [pl.ds(b * seq, seq) for b in range(n_seq)]
        scores = []
        for rs in rss:
            kk = qkv[rs, pl.ds(pl.multiple_of(qdim + kvh * 128, 128), 128)]
            qq = jnp.concatenate([qkv[rs, c] for c in qcols], axis=0)
            scores.append(lax.dot_general(qq, kk, (((1,), (1,)), ((), ())), preferred_element_type=F32))
        nxt = None if unit is None else project(unit)
        probs = []
        for s in scores:
            s = jnp.where(causal, s * 128 ** -0.5, -jnp.inf)
            e = jnp.exp(s - jnp.max(s, axis=-1, keepdims=True))
            probs.append((e * (1.0 / jnp.sum(e, axis=-1, keepdims=True))).astype(BF16))
        for rs, p in zip(rss, probs):
            vv = qkv[rs, pl.ds(pl.multiple_of(qdim + (kv_heads + kvh) * 128, 128), 128)]
            o = jnp.dot(p, vv, preferred_element_type=F32).astype(BF16)
            for i, c in enumerate(qcols):
                qkv[rs, c] = o[i * seq:(i + 1) * seq]
        return nxt

    @pl.loop(0, kv_heads // 2 - 1)
    def _(i):
        nxt = [attend(2 * i + m, 2 * i + 2 + m) for m in range(2)]
        for m in range(2):
            qkv[:, cols(2 * i + 2 + m)] = nxt[m]
        for m in range(2):
            start(2 * i + 2 + m + SLOTS, SLOTS + 2, SLOTS + n_qu - 1)

    for m in range(2):
        attend(jnp.int32(kv_heads - 2 + m), None)

    def wo_body(t, w0, w1):
        acc = jnp.dot(qkv[:, :half_q], w0[...], preferred_element_type=F32)
        acc += jnp.dot(qkv[:, half_q:qdim], w1[...], preferred_element_type=F32)
        h[:, cols(t)] = (h[:, cols(t)].astype(F32) + acc).astype(BF16)

    phase(u_wo, dim // WN, wo_body, 2)
    norm_rows(mlp_g)

    def gu_body(t, w0, w1):
        g = jnp.dot(a[...], w0[...], preferred_element_type=F32)
        u = jnp.dot(a[...], w1[...], preferred_element_type=F32)
        act[:, cols(t)] = (silu(g) * u).astype(BF16)

    phase(u_gu, ff // WN, gu_body, 2)

    def dn_body(t, *ws):
        acc = None
        for (s, n), w in zip(chunks(ff), ws):
            d = jnp.dot(act[:, s:s + n], w[...], preferred_element_type=F32)
            acc = d if acc is None else acc + d
        h[:, cols(t)] = (h[:, cols(t)].astype(F32) + acc).astype(BF16)

    phase(u_dn, dim // WN, dn_body)
    norm_rows(mamba_g)

    row_id = lax.broadcasted_iota(jnp.int32, (seq, 1), 0)

    def scatter(dst, r0, t, val):
        for j in range(WN // 128):
            for i in range(seq // 8):
                dst[pl.ds((r0 + i * 8) * PITCH + t * (WN // 128) + j, 8, stride=PITCH), :] = (
                    val[i * 8:(i + 1) * 8, j * 128:(j + 1) * 128])

    conv_pitch = seq + 8
    for k in range(2 * n_seq * (WN // 128)):
        delta[k * conv_pitch:k * conv_pitch + 8, :] = jnp.zeros((8, 128), F32)

    def wx_body(t, w, parity=0):
        res = jnp.dot(a[...], w[...], preferred_element_type=F32).astype(BF16).astype(F32)
        for b in range(n_seq):
            for j in range(WN // 128):
                top = ((parity * n_seq + b) * (WN // 128) + j) * conv_pitch + 8
                cj = pl.ds(pl.multiple_of(t * WN, WN) + j * 128, 128)
                xi = res[b * seq:(b + 1) * seq, j * 128:(j + 1) * 128]
                delta[top:top + seq, :] = xi
                acc = chan[4:5, cj] + chan[CONV - 1:CONV, cj] * xi
                for k in range(CONV - 1):
                    back = CONV - 1 - k
                    acc += chan[k:k + 1, cj] * delta[top - back:top - back + seq, :]
                c = silu(acc).astype(BF16)
                act[b * seq:(b + 1) * seq, cj] = c
                cf = c.astype(F32)
                for i in range(seq // 8):
                    xs[pl.ds((b * seq + i * 8) * PITCH + t * (WN // 128) + j, 8, stride=PITCH), :] = cf[i * 8:(i + 1) * 8]

    phase(u_wx, inner // WN, wx_body, 2)

    in_copies[0].wait()
    r = lax.dot_general(act[:, :inner], wxp[...], (((1,), (1,)), ((), ())), preferred_element_type=F32)
    n_r = r.shape[1]
    gain_r = jnp.concatenate([dt_g[...].reshape(1, dt_rank), b_g[...].reshape(1, n_state), c_g[...].reshape(1, n_state)], axis=1)
    col = lax.broadcasted_iota(jnp.int32, (1, n_r), 1)
    sq = r * r

    def inv_of(mask, n):
        return lax.rsqrt(jnp.sum(jnp.where(mask, sq, 0.0), axis=-1, keepdims=True) * (1.0 / n) + EPS)

    m_dt = col < dt_rank
    m_b = (col >= dt_rank) & (col < dt_rank + n_state)
    m_c = col >= dt_rank + n_state
    inv = jnp.where(m_dt, inv_of(m_dt, dt_rank), jnp.where(m_b, inv_of(m_b, n_state), inv_of(m_c, n_state)))
    rn = r * inv * gain_r
    rn_ref[...] = rn
    dt_in = rn[:, :dt_rank].astype(BF16)
    act[:, inner:inner + dt_rank] = dt_in
    in_copies[1].wait()

    def wz_body(t, w):
        pre = jnp.dot(act[:, inner:inner + dt_rank], wdt[:, cols(t)], preferred_element_type=F32)
        qkv[:, cols(t)] = jnp.dot(a[...], w[...], preferred_element_type=F32).astype(BF16)
        pre = pre + chan[5:6, cols(t)]
        step = jnp.maximum(pre, 0.0) + jnp.log1p(jnp.exp(-jnp.abs(pre)))
        for b in range(n_seq):
            scatter(delta, b * seq, t, step[b * seq:(b + 1) * seq])

    phase(u_wz, inner // WN, wz_body, 2)

    def bcast(ref, idx):
        return jnp.broadcast_to(ref[pl.ds(idx, 1), :], (8, 128))

    toks = 16

    for b in range(n_seq):
        for n in range(n_state):
            for ref, c0 in ((bb, dt_rank + n), (cb, dt_rank + n_state + n)):
                ref[n * seq:(n + 1) * seq, :] = jnp.broadcast_to(rn_ref[b * seq:(b + 1) * seq, c0:c0 + 1], (seq, 128))

        @pl.loop(0, lanes // 8)
        def _(c, b=b):
            av = [a2[pl.ds(n * PITCH + c * 8, 8), :] for n in range(n_state)]
            dsk = dskip[pl.ds(pl.multiple_of(c * 8, 8), 8), :]

            def tokens(i, st):
                st = list(st)
                for k in range(toks):
                    r = i * toks + k
                    at = pl.ds((b * seq + r) * PITCH + c * 8, 8)
                    d = delta[at, :]
                    x = xs[at, :]
                    dx = d * x
                    terms = []
                    for n in range(n_state):
                        st[n] = jnp.exp2(d * av[n]) * st[n] + dx * bcast(bb, n * seq + r)
                        terms.append(st[n] * bcast(cb, n * seq + r))
                    terms.append(dsk * x)
                    while len(terms) > 1:
                        terms = [terms[m] + terms[m + 1] for m in range(0, len(terms) - 1, 2)] + (
                            [terms[-1]] if len(terms) % 2 else [])
                    delta[at, :] = terms[0]
                return tuple(st)

            st = tuple(jnp.zeros((8, 128), F32) for _ in range(n_state))
            lax.fori_loop(0, seq // toks, tokens, st)

        @pl.loop(0, seq // 16)
        def _(i, b=b):
            r0 = pl.multiple_of(b * seq + i * 16, 16)
            for j in range(lanes):
                y = jnp.concatenate([delta[pl.ds((r0 + 8 * m) * PITCH + j, 8, stride=PITCH), :] for m in range(2)], axis=0)
                z = qkv[pl.ds(r0, 16), j * 128:(j + 1) * 128].astype(F32)
                act[pl.ds(r0, 16), j * 128:(j + 1) * 128] = (y * silu(z)).astype(BF16)

        rs = pl.ds(b * seq, seq)
        n_t = dim // WN
        if b == 0:
            for t in range(n_t):
                for j, (s, n) in enumerate(chunks(inner)):
                    copy((wout, s, n), 0, (u_out + 2 * t + j) % SLOTS).wait()
        for t in range(n_t):
            ct = pl.ds(t * WN, WN)
            ds = [jnp.dot(act[rs, s:s + n], ring[(u_out + 2 * t + j) % SLOTS, :n], preferred_element_type=F32)
                  for j, (s, n) in enumerate(chunks(inner))]
            a[rs, ct] = (h[rs, ct].astype(F32) + (ds[0] + ds[1])).astype(BF16)
            exchange(lambda p, b: a.at[blk(p, b), ct], lambda p, b: out_ref.at[p * n_seq + b, :, ct], 1, [b])

    exchange_wait(out_ref, a.at[pl.ds(0, rows - n_seq * tok)], 1)


def layer_pair(hidden, attn_norm, w_q, w_k, w_v, w_o, mlp_norm, w_gate, w_up, w_down, mamba_norm, w_in_x, w_in_z, conv_w, conv_b, w_xproj, dt_norm, b_norm, c_norm, w_dt, dt_bias, a_log, d_skip, w_out):
    n_batch, tok, dim = hidden.shape
    n_seq = n_batch // lax.axis_size("sp")
    rows = n_batch * tok
    inner, n_state = a_log.shape
    hbm = pl.BlockSpec(memory_space=pltpu.HBM)
    vm = pl.BlockSpec(memory_space=pltpu.VMEM)
    qkv_dim = (w_q.shape[1] + w_k.shape[1] + w_v.shape[1]) * 128
    return pl.pallas_call(
        block_kernel,
        out_shape=jax.ShapeDtypeStruct(hidden.shape, BF16),
        in_specs=[hbm] * 13 + [vm] * 11,
        out_specs=hbm,
        scratch_shapes=[
            pltpu.VMEM((SLOTS, dim, WN), BF16),
            pltpu.VMEM((STAGE, KB, 32, 128), BF16),
            pltpu.VMEM((rows, qkv_dim), BF16),
            pltpu.VMEM((rows, dim), BF16),
            pltpu.VMEM((rows, dim), BF16),
            pltpu.VMEM((rows, w_gate.shape[1]), BF16),
            pltpu.VMEM((rows * PITCH, 128), F32),
            pltpu.VMEM((rows * PITCH, 128), F32),
            pltpu.VMEM((128 * n_state, 128), F32),
            pltpu.VMEM((128 * n_state, 128), F32),
            pltpu.VMEM((w_xproj.shape[1], inner), BF16),
            pltpu.VMEM(w_dt.shape, BF16),
            pltpu.VMEM((n_state * PITCH, 128), F32),
            pltpu.VMEM((8, inner), F32),
            pltpu.VMEM((rows, w_xproj.shape[1]), F32),
            pltpu.SemaphoreType.DMA((SLOTS,)),
            pltpu.SemaphoreType.DMA((STAGE,)),
            pltpu.SemaphoreType.DMA((2,)),
            pltpu.SemaphoreType.DMA((2,)),
            pltpu.SemaphoreType.DMA((2,)),
        ],
        compiler_params=pltpu.CompilerParams(vmem_limit_bytes=67043328, collective_id=0, has_side_effects=True),
        name="block",
    )(hidden, w_q.reshape(-1, 32, 128), w_k.reshape(-1, 32, 128), w_v.reshape(-1, 32, 128), w_o.reshape(-1, dim),
      w_gate, w_up, w_down, w_in_x, w_in_z, w_xproj.T, w_dt, w_out, attn_norm, mlp_norm, mamba_norm, conv_w, conv_b,
      dt_norm, b_norm, c_norm, dt_bias, d_skip.reshape(-1, 128), a_log.T)


def solution(mesh):
    act_spec = P("dp", "sp", None)
    return jax.shard_map(
        layer_pair,
        mesh=mesh,
        in_specs=(act_spec,) + (P(),) * 23,
        out_specs=act_spec,
        check_vma=False,
    )
```
